32 devices in a mesh: dp: 16 (over z, x, core), emb: 2 (over y).
Axes of the slice: x: 2, y: 2, z: 4, core: 2. Of those that a mesh axis runs over, the one named last changes fastest.
Arguments:
- cur_ids: int32 [8192], P(('dp', 'emb')), may hold values from 0 to 3071, as said below
- prev_ids: int32 [8192], P(('dp', 'emb')), may hold values from 0 to 3071, as said below
- prev_grads: bfloat16 [8192, 128], P(('dp', 'emb')), may hold values from -6 to 6
- row_place: int32 [3072], replicated, may hold values from 0 to 3071, as said below
- table: float32 [3072, 128], P('emb'), may hold values from -6 to 6
- accum: float32 [3072, 128], P('emb'), may hold values from 0.05 to 2
- labels: float32 [8192], P('dp'), may hold values from 0 to 1
- gain: float32 [128], replicated, may hold values from 0.5 to 1.5
- w_gate: bfloat16 [128, 4096], P(None, 'emb'), may hold values from -0.5 to 0.5
- w_up: bfloat16 [128, 4096], P(None, 'emb'), may hold values from -0.5 to 0.5
- w_out: bfloat16 [4096], P('emb'), may hold values from -0.09375 to 0.09375
Outputs:
- new_table: float32 [3072, 128], P('emb')
- new_accum: float32 [3072, 128], P('emb')
- grad_gate: float32 [128, 4096], P(None, 'emb')
- grad_up: float32 [128, 4096], P(None, 'emb')
- emb_grad: float32 [8192, 128], P(('dp', 'emb'))
The draws below stay inside these ranges and needn't reach their ends.
Inputs may be any that keep to these rules, and one draw needn't show every extreme that they name: A permutation of the table rows; row i is stored on shard row_place[i] // 1536 of emb at position row_place[i] % 1536. `cur_ids`: the 256 ids of one device name rows of one shard at most 256 times, and exactly 256 times for some shard. `prev_ids`: the 256 ids of one device name rows of one shard at most 256 times, and exactly 256 times for some shard.
All inputs are finite; a program needn't handle non-finite values.
Results may differ from the reference program's by a relative error of at most 0.0069.
Values may be sent and summed in bfloat16 or wider, within the bound.
A program may use at most 64 MiB of HBM per device.

```python
import math
import jax
import jax.numpy as jnp
from jax import lax

E = 128
HID = 4096
TOK_DEV = 256
ROWS_SHARD = 1536
TOKENS = 8192
VOCAB = 3072
CAP = 256
N_DP = 16
N_EMB = 2


def place_table(key):
    return jax.random.permutation(jax.random.fold_in(key, 11), VOCAB).astype(jnp.int32)


def draw_ids(key, salt):
    placement = place_table(key)
    inverse = jnp.zeros((VOCAB,), jnp.int32).at[placement].set(jnp.arange(VOCAB, dtype=jnp.int32))
    blocks = TOKENS // TOK_DEV
    salted = jax.random.fold_in(key, salt)
    hot_shard = jax.random.randint(jax.random.fold_in(salted, 1), (blocks, 1), 0, N_EMB)
    position = jnp.arange(TOK_DEV, dtype=jnp.int32)[None, :]
    others = (hot_shard + 1 + (position - CAP) % max(N_EMB - 1, 1)) % N_EMB
    target = jnp.where(position < CAP, hot_shard, others)
    device_keys = jax.random.split(jax.random.fold_in(salted, 2), blocks)
    shuffle = jax.vmap(lambda one_key: jax.random.permutation(one_key, TOK_DEV))(device_keys)
    target = jnp.take_along_axis(target, shuffle, axis=1)
    first_pick = jax.random.randint(jax.random.fold_in(salted, 3), (blocks, TOK_DEV), 0, ROWS_SHARD)
    second_pick = jax.random.randint(jax.random.fold_in(salted, 4), (blocks, TOK_DEV), 0, ROWS_SHARD)
    slot_index = jnp.minimum(first_pick, second_pick)
    return inverse[target * ROWS_SHARD + slot_index].reshape(TOKENS).astype(jnp.int32)


def draw_row_place(key, part):
    return place_table(key)


def draw_cur_ids(key, part):
    return draw_ids(key, 21)


def draw_prev_ids(key, part):
    return draw_ids(key, 22)


def level_of(key, shape, cuts, smallest, top_value):
    def one(dim, blocks):
        steps = jax.random.uniform(jax.random.fold_in(jax.random.fold_in(key, 6), dim), (blocks,), jnp.float32, smallest / len(cuts), top_value / len(cuts))
        return jnp.repeat(jnp.exp(steps), shape[dim] // blocks).reshape((-1,) + (1,) * (len(shape) - dim - 1))

    factor_of = one(*cuts[0])
    for cut in cuts[1:]:
        factor_of = factor_of * one(*cut)
    return factor_of


def normal_values(rng, dims, deviation, reach, pieces=(), held_as=jnp.bfloat16):
    entries = deviation * jax.random.normal(rng, dims, jnp.float32)
    if pieces:
        entries = entries * level_of(rng, dims, pieces, -0.22, 0.18)
    return jnp.clip(entries, -reach, reach).astype(held_as)


def setup_inputs(seed: int = 0) -> dict:
    key_of = jax.random.split(jax.random.key(seed), 12)
    cur_ids = draw_cur_ids(jax.random.fold_in(key_of[11], 71), 0)
    prev_ids = draw_prev_ids(jax.random.fold_in(key_of[11], 71), 0)
    prev_grads = normal_values(key_of[2], (TOKENS, E), 1.0, 6.0, ((0, 32),))
    row_place = draw_row_place(jax.random.fold_in(key_of[11], 71), 0)
    table = normal_values(key_of[4], (VOCAB, E), 1.0, 6.0, ((0, 2),), jnp.float32)
    accum = jnp.clip(jnp.exp(math.log(2.0) - 3.6888794 * jax.random.uniform(key_of[5], (VOCAB, E), jnp.float32) ** level_of(key_of[5], (VOCAB, E), ((0, 2),), -0.2, 0.2)), 0.05, 2.0)
    labels = jnp.clip(1.0 * jax.random.uniform(key_of[6], (TOKENS,), jnp.float32) ** level_of(key_of[6], (TOKENS,), ((0, 16),), -0.2, 0.2), 0.0, 1.0)
    gain = jnp.clip(1.0 + 0.1 * jax.random.normal(key_of[7], (E,), jnp.float32), 0.5, 1.5)
    w_gate = normal_values(key_of[8], (E, HID), E ** -0.5, 0.5, ((1, 2),))
    w_up = normal_values(key_of[9], (E, HID), E ** -0.5, 0.5, ((1, 2),))
    w_out = normal_values(key_of[10], (HID,), HID ** -0.5, 0.09375, ((0, 2),))
    return {"cur_ids": cur_ids, "prev_ids": prev_ids, "prev_grads": prev_grads, "row_place": row_place, "table": table, "accum": accum, "labels": labels, "gain": gain, "w_gate": w_gate, "w_up": w_up, "w_out": w_out}


loss_weight = 64.0
learn_rate = 0.1
norm_eps = 1e-06

def reference(cur_ids, prev_ids, prev_grads, row_place, table, accum, labels, gain, w_gate, w_up, w_out):
    gain_f = gain.astype(jnp.float32)

    def tower_block(sums_so_far, blocked):
        positions, targets = blocked
        looked_up = table[positions].astype(jnp.bfloat16)
        values = looked_up.astype(jnp.float32)
        inverse_rms = lax.rsqrt(lax.optimization_barrier(jnp.mean(values * values, axis=1, keepdims=True)) + norm_eps)
        normed = (values * inverse_rms * gain_f).astype(jnp.bfloat16)
        gate_proj = jnp.dot(normed, w_gate, preferred_element_type=jnp.float32)
        up_proj = jnp.dot(normed, w_up, preferred_element_type=jnp.float32)
        sigmoid_gate = jax.nn.sigmoid(gate_proj)
        activated = gate_proj * sigmoid_gate
        hidden = (activated * up_proj).astype(jnp.bfloat16)
        logits = jnp.dot(hidden, w_out, preferred_element_type=jnp.float32)
        slopes = loss_weight * (jax.nn.sigmoid(logits) - targets)
        back_hidden = slopes[:, None] * w_out.astype(jnp.float32)[None, :]
        back_gate = (back_hidden * up_proj * sigmoid_gate * (1.0 + gate_proj * (1.0 - sigmoid_gate))).astype(jnp.bfloat16)
        back_up = (back_hidden * activated).astype(jnp.bfloat16)
        contract = (((0,), (0,)), ((), ()))
        gate_part = lax.dot_general(normed, back_gate, contract, preferred_element_type=jnp.float32)
        up_part = lax.dot_general(normed, back_up, contract, preferred_element_type=jnp.float32)
        across = (((1,), (1,)), ((), ()))
        back_normed = lax.dot_general(back_gate, w_gate, across, preferred_element_type=jnp.float32)
        back_normed = back_normed + lax.dot_general(back_up, w_up, across, preferred_element_type=jnp.float32)
        scaled = back_normed * gain_f
        row_grad = inverse_rms * scaled - values * inverse_rms ** 3 * lax.optimization_barrier(jnp.mean(values * scaled, axis=1, keepdims=True))
        return ((sums_so_far[0] + gate_part, sums_so_far[1] + up_part), row_grad)
    positions = row_place[cur_ids].reshape(N_DP, -1)
    targets = labels.reshape(N_DP, -1)
    start_sums = (jnp.zeros((E, HID), jnp.float32), jnp.zeros((E, HID), jnp.float32))
    (gate_sum, up_sum), row_grads = lax.scan(tower_block, start_sums, (positions, targets))
    tower_scale = 1.0 / math.sqrt(TOKENS)
    table_grad = jax.ops.segment_sum(prev_grads.astype(jnp.float32), row_place[prev_ids], num_segments=VOCAB)
    new_accum = accum + table_grad * table_grad
    new_table = table - learn_rate * table_grad * lax.rsqrt(new_accum)
    return (new_table, new_accum, gate_sum * tower_scale, up_sum * tower_scale, row_grads.reshape(TOKENS, E))
```

```python
import functools
import math

import jax
import jax.numpy as jnp
from jax import lax
from jax.experimental import pallas as pl
from jax.experimental.pallas import tpu as pltpu
from jax.sharding import PartitionSpec as P

loss_weight = 64.0
learn_rate = 0.1
norm_eps = 1e-06
MESH = pl.DeviceIdType.MESH
F32 = jnp.float32
BF16 = jnp.bfloat16
LANES = 128


def dot(a, b):
    return jnp.dot(a, b, preferred_element_type=F32)


def dot_nt(a, b):
    return lax.dot_general(a, b, (((1,), (1,)), ((), ())), preferred_element_type=F32)


class Reduce:
    def __init__(self, at, copy, pending, bufs, send, recv):
        self.at, self.copy, self.pending = at, copy, pending
        self.part, self.pair, self.x_out, self.keep, self.x_in, self.z_out, self.z_in, self.full = bufs
        self.send, self.recv = send, recv
        self.half = self.pair.shape[0]
        self.quarter = self.half // 2
        self.size = self.quarter // at["n_hi"]

    def rows(self, start, size):
        return pl.ds(pl.multiple_of(start, math.gcd(size, 128)), size)

    def place(self, lo, hi):
        return self.rows(self.at["par"] * self.half + lo * self.quarter + hi * self.size, self.size)

    def go(self, src, dst, stage, k, dp):
        one = self.copy(src, dst, self.send.at[stage, k], self.recv.at[stage, k], dp, self.at["emb"])
        one.start()
        self.pending.append(one)
        return one

    def start(self, away):
        lo = 1 - self.at["low"] if away else self.at["low"]
        src = self.rows((1 - self.at["par"]) * self.half + lo * self.quarter, self.quarter)
        dst = self.rows(lo * self.quarter, self.quarter)
        one = self.go(self.part.at[src], self.pair.at[dst], 0, 0 if away else 1, self.at["partner"])
        if away:
            self.first_away = one
        else:
            self.first_keep = one

    def stage_x(self):
        at = self.at
        self.first_away.wait_recv()
        self.x = {}
        lo = (1 - at["low"]) * self.quarter
        for k in list(range(1, at["n_hi"])) + [0]:
            piece = at["ahead"][k] * self.size
            mine = self.part[self.rows(at["par"] * self.half + lo + piece, self.size), :]
            theirs = self.pair[self.rows(lo + piece, self.size), :]
            self.x_out[k] = (mine.astype(F32) + theirs.astype(F32)).astype(BF16)
            self.x[k] = self.go(self.x_out.at[k], self.x_in.at[k], 1, k, at["beside"])

    def stage_keep(self):
        at = self.at
        self.first_keep.wait_recv()
        lo = at["low"] * self.quarter
        mine = self.part[self.rows(at["par"] * self.half + lo, self.quarter), :]
        theirs = self.pair[self.rows(lo, self.quarter), :]
        self.keep[...] = mine.astype(F32) + theirs.astype(F32)

    def joined(self, k):
        self.x[k].wait_recv()
        kept = self.keep[self.rows(self.at["ahead"][k] * self.size, self.size), :]
        return kept + self.x_in[k].astype(F32)

    def stage_z(self):
        self.z = []
        for k in range(1, self.at["n_hi"]):
            self.z_out[k - 1] = self.joined(k).astype(BF16)
            self.z.append(
                self.go(self.z_out.at[k - 1], self.z_in.at[k - 1], 2, k, self.at["far"][k])
            )

    def stage_sum(self):
        at = self.at
        total = self.joined(0)
        for k, one in enumerate(self.z):
            one.wait_recv()
            total = total + self.z_in[k].astype(F32)
        mine = self.place(at["low"], at["high"])
        self.full[mine, :] = total.astype(BF16)
        view = self.full.at[mine]
        self.spread = [self.go(view, view, 3, k, at["far"][k]) for k in range(1, at["n_hi"])]
        self.near = [self.go(view, view, 4, 0, at["beside"])]
        self.last = [self.go(view, view, 5, 0, at["partner"])]

    def spread_z(self):
        at = self.at
        for k in range(1, at["n_hi"]):
            self.spread[k - 1].wait_recv()
            view = self.full.at[self.place(at["low"], at["behind"][k])]
            self.near.append(self.go(view, view, 4, k, at["beside"]))
            self.last.append(self.go(view, view, 5, k, at["partner"]))

    def spread_x(self):
        at = self.at
        n_hi = at["n_hi"]
        for k in range(n_hi):
            self.near[k].wait_recv()
            view = self.full.at[self.place(1 - at["low"], at["behind"][k])]
            self.last.append(self.go(view, view, 5, n_hi + k, at["partner"]))

    def finish(self):
        for one in self.last:
            one.wait_recv()


def tower_kernel(
    n_dp,
    n_emb,
    scale,
    cur_ref,
    prev_ref,
    grads_ref,
    place_ref,
    table_ref,
    labels_ref,
    gain_ref,
    wg_ref,
    wu_ref,
    wo_ref,
    total_ref,
    tower_ref,
    emb_ref,
    ids,
    gall,
    place,
    table,
    labels,
    gain,
    wg,
    wu,
    wo,
    table16,
    wo_row,
    scaled_w,
    contrib,
    lbuf,
    values,
    normed,
    normed_t,
    act,
    logit_acc,
    logit,
    logit_in,
    slopes,
    lead,
    bn,
    bn_in,
    tpart,
    tpair,
    tx_out,
    tkeep,
    tx_in,
    tz_out,
    tz_in,
    tall,
    gpart,
    gpair,
    gx_out,
    gkeep,
    gx_in,
    gz_out,
    gz_in,
    gall_sum,
    load,
    e_send,
    e_recv,
    t_send,
    t_recv,
    g_send,
    g_recv,
):
    me_dp = lax.axis_index("dp")
    me_emb = lax.axis_index("emb")
    n_chip = n_dp // 2
    n_hi = n_chip // 2
    chip = me_dp // 2
    low = chip % 2
    high = chip // 2
    par = me_dp % 2
    partner = me_dp + 1 - 2 * par
    beside = me_dp + 2 - 4 * low
    tok = gall.shape[1]
    rows = table.shape[0]
    hid = wg.shape[1]
    ht = 256
    tiles = hid // ht

    def copy(src, dst, send, recv, dp, emb):
        return pltpu.make_async_remote_copy(
            src_ref=src,
            dst_ref=dst,
            send_sem=send,
            recv_sem=recv,
            device_id=(dp, emb),
            device_id_type=MESH,
        )

    def other_emb(k):
        return lax.rem(me_emb + k, n_emb)

    def tokens(e):
        return pl.ds(pl.multiple_of(e * tok, tok), tok)

    ahead = [lax.rem(high + k, n_hi) for k in range(n_hi)]
    behind = [lax.rem(high + n_hi - k, n_hi) for k in range(n_hi)]
    far = [(2 * h + low) * 2 + par for h in ahead]
    at = dict(
        n_hi=n_hi, par=par, low=low, high=high, partner=partner, beside=beside,
        ahead=ahead, behind=behind, far=far, emb=me_emb,
    )
    pending = []
    sums = Reduce(
        at, copy, pending, (tpart, tpair, tx_out, tkeep, tx_in, tz_out, tz_in, tall), t_send, t_recv
    )
    tower = Reduce(
        at, copy, pending, (gpart, gpair, gx_out, gkeep, gx_in, gz_out, gz_in, gall_sum), g_send, g_recv
    )

    barrier = pltpu.get_barrier_semaphore()
    for k in range(1, n_emb):
        pl.semaphore_signal(barrier, inc=1, device_id=(me_dp, other_emb(k)), device_id_type=MESH)
    for peer in far[1:] + [beside, partner]:
        pl.semaphore_signal(barrier, inc=1, device_id=(peer, me_emb), device_id_type=MESH)

    loads = []
    for i, (src, dst) in enumerate(
        [
            (cur_ref, ids.at[me_emb, 0]),
            (prev_ref, ids.at[me_emb, 1]),
            (place_ref, place),
            (grads_ref, gall.at[me_emb]),
            (table_ref, table),
            (wo_ref, wo),
            (wg_ref, wg),
            (wu_ref, wu),
            (gain_ref, gain),
            (labels_ref, labels),
        ]
    ):
        one = pltpu.make_async_copy(src, dst, load.at[i])
        one.start()
        loads.append(one)
    loads[0].wait()
    loads[1].wait()
    pl.semaphore_wait(barrier, n_emb - 1 + n_hi - 1 + 2)

    def to_peers(src, dst_of, stage, slot, peers=None):
        sent = []
        for k in peers or range(1, n_emb):
            one = copy(
                src(k), dst_of(k), e_send.at[stage, slot, k - 1], e_recv.at[stage, slot, k - 1], me_dp, other_emb(k)
            )
            one.start()
            sent.append(one)
        pending.extend(sent)
        return sent

    own_ids = ids.at[me_emb]
    id_copies = to_peers(lambda k: own_ids, lambda k: own_ids, 0, 0)
    loads[3].wait()
    own_grads = gall.at[me_emb]
    grad_copies = to_peers(lambda k: own_grads, lambda k: own_grads, 1, 0)

    loads[2].wait()
    groups = place.shape[0]
    stored = place[...]
    digits = jnp.concatenate([stored >> 6, stored & 63], axis=0).astype(F32).astype(BF16)

    def place_of(wanted):
        lane = lax.broadcasted_iota(jnp.int32, (LANES, tok), 0)
        hot = jnp.where(lane == (wanted & (LANES - 1)), 1.0, 0.0).astype(BF16)
        found = dot(digits, hot)
        found = found[0:groups, :] * 64.0 + found[groups : 2 * groups, :]
        group = lax.broadcasted_iota(jnp.int32, (groups, tok), 0)
        picked = jnp.where(group == (wanted >> 7), found, 0.0)
        return jnp.sum(picked, axis=0, keepdims=True).astype(jnp.int32)

    base = me_emb * rows
    kt = 256
    prev_pos = []

    loads[4].wait()
    table16[...] = table[...].astype(BF16)

    row_copies = {}
    for s in range(n_emb):
        e = other_emb(s)
        if s > 0:
            id_copies[n_emb - s - 1].wait_recv()
        line = jnp.broadcast_to(place_of(ids[e, 0]) - base, (LANES, tok)).T
        line = jnp.concatenate([line] * (kt // LANES), axis=1)
        acc = jnp.zeros((tok, LANES), F32)
        for i in range(rows // kt):
            index = lax.broadcasted_iota(jnp.int32, (tok, kt), 1) + i * kt
            hot = jnp.where(index == line, 1.0, 0.0).astype(BF16)
            acc = acc + dot(hot, table16[i * kt : (i + 1) * kt, :])
        view = contrib.at[tokens(e)]
        contrib[tokens(e), :] = acc.astype(BF16)
        for k, one in zip(
            range(1, n_emb), to_peers(lambda k: view, lambda k: lbuf.at[k - 1, tokens(e)], 2, s)
        ):
            row_copies[k, s] = one
        prev_pos.append((e, place_of(ids[e, 1]) - base))

    for one in grad_copies:
        one.wait_recv()
    half_rows = rows // 2
    pt = 128 if half_rows % 128 == 0 else half_rows

    def grad_half(which):
        def grad_step(i, carry):
            at_row = pl.multiple_of(which * half_rows + i * pt, pt)
            index = lax.broadcasted_iota(jnp.int32, (pt, tok), 0) + at_row
            acc = jnp.zeros((pt, LANES), F32)
            for e, pos in prev_pos:
                hot = jnp.where(index == pos, 1.0, 0.0).astype(BF16)
                acc = acc + dot(hot, gall[e])
            tpart[pl.ds(at_row, pt), :] = acc
            return carry

        lax.fori_loop(0, half_rows // pt, grad_step, 0)

    grad_half(1 - par)
    sums.start(True)
    sums.start(False)
    grad_half(par)
    for one in loads[5:]:
        one.wait()
    wo_row[...] = wo[...].astype(F32)
    per_tile = ht // LANES

    def head_of(j):
        parts = [wo_row[pl.ds(j * per_tile + b, 1), :] for b in range(per_tile)]
        return jnp.concatenate(parts, axis=1)

    sums.stage_x()

    def scale_step(j, carry):
        cols = pl.ds(pl.multiple_of(j * ht, ht), ht)
        head = head_of(j)
        scaled_w[0, :, cols] = (wg[:, cols].astype(F32) * head).astype(BF16)
        scaled_w[1, :, cols] = (wu[:, cols].astype(F32) * head).astype(BF16)
        return carry

    lax.fori_loop(0, tiles, scale_step, 0)
    sums.stage_keep()

    def forward(e):
        span = tokens(e)
        looked = contrib[span, :].astype(F32)
        for k in range(1, n_emb):
            looked = looked + lbuf[k - 1, span, :].astype(F32)
        values[span, :] = looked
        inverse_rms = lax.rsqrt(jnp.mean(looked * looked, axis=1, keepdims=True) + norm_eps)
        norm = (looked * inverse_rms * gain[...]).astype(BF16)
        normed[span, :] = norm
        normed_t[:, span] = norm.astype(F32).T
        logit_acc[...] = jnp.zeros_like(logit_acc)

        def tower_step(j, carry):
            cols = pl.ds(pl.multiple_of(j * ht, ht), ht)
            gate = dot(normed[span, :], wg[:, cols])
            up = dot(normed[span, :], wu[:, cols])
            sig = 0.5 + 0.5 * jnp.tanh(0.5 * gate)
            activated = gate * sig
            act[0, span, cols] = (up * (sig + activated * (1.0 - sig))).astype(BF16)
            act[1, span, cols] = activated.astype(BF16)
            weighed = activated * up * head_of(j)
            part = weighed[:, 0:LANES]
            for b in range(1, per_tile):
                part = part + weighed[:, b * LANES : (b + 1) * LANES]
            logit_acc[...] += part
            return carry

        lax.fori_loop(0, tiles, tower_step, 0)
        logit[e] = jnp.sum(logit_acc[...].T, axis=0, keepdims=True)

    def backward(e):
        span = tokens(e)

        def back_step(j, carry):
            cols = pl.ds(pl.multiple_of(j * ht, ht), ht)
            return carry + dot_nt(act[0, span, cols], scaled_w[0, :, cols]) + dot_nt(
                act[1, span, cols], scaled_w[1, :, cols]
            )

        bn[span, :] = lax.fori_loop(0, tiles, back_step, jnp.zeros((tok, LANES), F32))

    logit_copies = []
    for q in range(1, n_emb + 1):
        e = other_emb(n_emb - q)
        for k in range(1, n_emb):
            row_copies[k, (k - q) % n_emb].wait_recv()
        forward(e)
        view = logit.at[e]
        logit_copies += to_peers(lambda k: view, lambda k: logit_in.at[k - 1, e], 3, q - 1)
        if q == 1:
            sums.stage_z()
    back_copies = []
    for q in range(1, n_emb):
        e = other_emb(n_emb - q)
        backward(e)
        k = n_emb - q
        view = bn.at[tokens(e)]
        back_copies += to_peers(lambda k: view, lambda k: bn_in.at[k - 1], 4, 0, [k])
    backward(me_emb)
    sums.stage_sum()

    for one in logit_copies:
        one.wait_recv()
    for e in range(n_emb):
        logits = logit[e]
        for k in range(n_emb - 1):
            logits = logits + logit_in[k, e]
        slope = loss_weight * (jax.nn.sigmoid(logits) - labels[e])
        slopes[e] = slope
        span = slice(e * tok, (e + 1) * tok)
        lead[:, span] = (normed_t[:, span] * slope).astype(BF16)

    def weight_grads(which, lo):
        def step(i, carry):
            j = lo * (tiles // 2) + i
            cols = pl.ds(pl.multiple_of(j * ht, ht), ht)
            part = (dot(lead[...], act[which, :, cols]) * (head_of(j) * scale)).astype(BF16)
            for b in range(per_tile):
                to = which * hid + j * ht + b * LANES
                gpart[pl.ds(pl.multiple_of(to, LANES), LANES), :] = part[:, b * LANES : (b + 1) * LANES]
            return carry

        lax.fori_loop(0, tiles // 2, step, 0)

    weight_grads(1 - par, 1 - low)
    tower.start(True)
    weight_grads(par, 1 - low)
    weight_grads(1 - par, low)
    tower.start(False)
    tower.stage_x()
    weight_grads(par, low)
    tower.stage_keep()
    sums.spread_z()

    for one in back_copies:
        one.wait_recv()
    own = tokens(me_emb)
    back = bn[own, :]
    for k in range(n_emb - 1):
        back = back + bn_in[k]
    slope_col = jnp.broadcast_to(slopes[me_emb], (LANES, tok)).T
    scaled = back * slope_col * gain[...]
    x = values[own, :]
    inv = lax.rsqrt(jnp.mean(x * x, axis=1, keepdims=True) + norm_eps)
    emb_ref[...] = inv * scaled - x * (inv * inv * inv) * jnp.mean(
        x * scaled, axis=1, keepdims=True
    )

    tower.stage_z()
    sums.spread_x()
    tower.stage_sum()
    sums.finish()
    total_ref[...] = tall[...]
    tower.spread_z()
    tower.spread_x()
    tower.finish()
    tower_ref[...] = gall_sum[...]
    for one in pending:
        one.wait_send()


def write_kernel(
    total_ref, table_ref, accum_ref, tower_ref, emb_ref,
    table_out, accum_out, gate_out, up_out, emb_out,
    new_table, new_accum, gate, up, sem,
):
    hid = gate.shape[1]
    rows = new_table.shape[0]
    sent = []

    def send(src, dst):
        one = pltpu.make_async_copy(src, dst, sem.at[len(sent)])
        one.start()
        sent.append(one)

    send(emb_ref, emb_out)
    n_col = 2
    for which, (buf, out) in enumerate(((gate, gate_out), (up, up_out))):
        for c in range(n_col):
            for b in range(c * hid // LANES // n_col, (c + 1) * hid // LANES // n_col):
                start = which * hid + b * LANES
                buf[:, b * LANES : (b + 1) * LANES] = tower_ref[start : start + LANES, :].astype(F32)
            cols = slice(c * hid // n_col, (c + 1) * hid // n_col)
            send(buf.at[:, cols], out.at[:, cols])
    n_row = 2
    for c in range(n_row):
        span = slice(c * rows // n_row, (c + 1) * rows // n_row)
        total = total_ref[span, :].astype(F32)
        grown = accum_ref[span, :] + total * total
        new_accum[span, :] = grown
        new_table[span, :] = table_ref[span, :] - learn_rate * total * lax.rsqrt(grown)
        send(new_accum.at[span], accum_out.at[span])
        send(new_table.at[span], table_out.at[span])
    for one in sent:
        one.wait()


def on_device(
    cur_ids, prev_ids, prev_grads, row_place, table, accum, labels, gain, w_gate, w_up, w_out
):
    n_emb = lax.axis_size("emb")
    n_dp = lax.axis_size("dp")
    n_chip = n_dp // 2
    n_hi = n_chip // 2
    rows, width = table.shape
    tok = cur_ids.shape[0]
    group = tok * n_emb
    hid = w_gate.shape[1]
    groups = row_place.shape[0] // LANES
    scale = 1.0 / math.sqrt(tok * n_emb * n_dp)
    vmem = pl.BlockSpec(memory_space=pltpu.VMEM)
    hbm = pl.BlockSpec(memory_space=pltpu.HBM)
    n_peer = max(n_emb - 1, 1)
    dma = pltpu.SemaphoreType.DMA
    I32 = jnp.int32

    def reduce_buffers(total_rows, dtype):
        half = total_rows // 2
        size = half // n_chip
        return [
            pltpu.VMEM((total_rows, width), dtype),
            pltpu.VMEM((half, width), dtype),
            pltpu.VMEM((n_hi, size, width), BF16),
            pltpu.VMEM((half // 2, width), F32),
            pltpu.VMEM((n_hi, size, width), BF16),
            pltpu.VMEM((n_hi - 1, size, width), BF16),
            pltpu.VMEM((n_hi - 1, size, width), BF16),
            pltpu.VMEM((total_rows, width), BF16),
        ]

    total, tower, emb_grad = pl.pallas_call(
        functools.partial(tower_kernel, n_dp, n_emb, scale),
        out_shape=(
            jax.ShapeDtypeStruct((rows, width), BF16),
            jax.ShapeDtypeStruct((2 * hid, width), BF16),
            jax.ShapeDtypeStruct((tok, width), F32),
        ),
        in_specs=[hbm] * 10,
        out_specs=(vmem,) * 3,
        scratch_shapes=[
            pltpu.VMEM((n_emb, 2, 1, tok), I32),
            pltpu.VMEM((n_emb, tok, width), BF16),
            pltpu.VMEM((groups, LANES), I32),
            pltpu.VMEM((rows, width), F32),
            pltpu.VMEM((n_emb, 1, tok), F32),
            pltpu.VMEM((1, width), F32),
            pltpu.VMEM((width, hid), BF16),
            pltpu.VMEM((width, hid), BF16),
            pltpu.VMEM((hid // LANES, LANES), BF16),
            pltpu.VMEM((rows, width), BF16),
            pltpu.VMEM((hid // LANES, LANES), F32),
            pltpu.VMEM((2, width, hid), BF16),
            pltpu.VMEM((group, width), BF16),
            pltpu.VMEM((n_peer, group, width), BF16),
            pltpu.VMEM((group, width), F32),
            pltpu.VMEM((group, width), BF16),
            pltpu.VMEM((width, group), F32),
            pltpu.VMEM((2, group, hid), BF16),
            pltpu.VMEM((tok, width), F32),
            pltpu.VMEM((n_emb, 1, tok), F32),
            pltpu.VMEM((n_peer, n_emb, 1, tok), F32),
            pltpu.VMEM((n_emb, 1, tok), F32),
            pltpu.VMEM((width, group), BF16),
            pltpu.VMEM((group, width), F32),
            pltpu.VMEM((n_peer, tok, width), F32),
        ]
        + reduce_buffers(rows, F32)
        + reduce_buffers(2 * hid, BF16)
        + [
            dma((10,)),
            dma((5, n_emb, n_peer)),
            dma((5, n_emb, n_peer)),
            dma((6, 2 * n_hi)),
            dma((6, 2 * n_hi)),
            dma((6, 2 * n_hi)),
            dma((6, 2 * n_hi)),
        ],
        compiler_params=pltpu.CompilerParams(
            collective_id=0, has_side_effects=True, vmem_limit_bytes=40 * 1024 * 1024
        ),
    )(
        cur_ids.reshape(1, -1),
        prev_ids.reshape(1, -1),
        prev_grads,
        row_place.reshape(-1, LANES),
        table,
        labels.reshape(n_emb, 1, -1),
        gain.reshape(1, -1),
        w_gate,
        w_up,
        w_out.reshape(-1, LANES),
    )
    return pl.pallas_call(
        write_kernel,
        out_shape=(
            jax.ShapeDtypeStruct((rows, width), F32),
            jax.ShapeDtypeStruct((rows, width), F32),
            jax.ShapeDtypeStruct((width, hid), F32),
            jax.ShapeDtypeStruct((width, hid), F32),
            jax.ShapeDtypeStruct((tok, width), F32),
        ),
        in_specs=[vmem] * 5,
        out_specs=(hbm,) * 5,
        scratch_shapes=[
            pltpu.VMEM((rows, width), F32),
            pltpu.VMEM((rows, width), F32),
            pltpu.VMEM((width, hid), F32),
            pltpu.VMEM((width, hid), F32),
            dma((9,)),
        ],
        compiler_params=pltpu.CompilerParams(vmem_limit_bytes=16 * 1024 * 1024),
    )(total, table, accum, tower, emb_grad)


def solution(mesh):
    placed = (
        P(("dp", "emb")),
        P(("dp", "emb")),
        P(("dp", "emb"), None),
        P(),
        P("emb", None),
        P("emb", None),
        P("dp"),
        P(),
        P(None, "emb"),
        P(None, "emb"),
        P("emb"),
    )
    return jax.shard_map(
        on_device,
        mesh=mesh,
        in_specs=placed,
        out_specs=(
            P("emb", None),
            P("emb", None),
            P(None, "emb"),
            P(None, "emb"),
            P(("dp", "emb"), None),
        ),
        check_vma=False,
    )
```

```python
import functools
import math

import jax
import jax.numpy as jnp
from jax import lax
from jax.experimental import pallas as pl
from jax.experimental.pallas import tpu as pltpu
from jax.sharding import PartitionSpec as P

loss_weight = 64.0
learn_rate = 0.1
norm_eps = 1e-06
MESH = pl.DeviceIdType.MESH
F32 = jnp.float32
BF16 = jnp.bfloat16
LANES = 128


def dot(a, b):
    return jnp.dot(a, b, preferred_element_type=F32)


def dot_nt(a, b):
    return lax.dot_general(a, b, (((1,), (1,)), ((), ())), preferred_element_type=F32)


class Reduce:
    def __init__(self, at, copy, bufs, send, recv):
        self.at, self.copy = at, copy
        self.part, self.pair, self.x_out, self.keep, self.x_in, self.z_out, self.z_in, self.full = bufs
        self.send, self.recv = send, recv
        self.half = self.pair.shape[0]
        self.quarter = self.half // 2
        n_hi = at["n_hi"]
        self.size = self.quarter // n_hi
        self.subs = subs_of(self.size)
        self.bits = [1 << b for b in reversed(range(n_hi.bit_length() - 1))]
        self.masks = sorted(range(1, n_hi), key=lambda m: (-(m & -m), m))
        self.base = recv_layout(n_hi, self.subs)[0]

    def rows(self, start, size):
        return pl.ds(pl.multiple_of(start, math.gcd(size, 128)), size)

    def place(self, lo, hi, sub=None):
        start = self.at["par"] * self.half + lo * self.quarter + hi * self.size
        if sub is None:
            return self.rows(start, self.size)
        step = self.size // self.subs
        return self.rows(start + sub * step, step)

    def go(self, src, dst, stage, k, dp):
        one = self.copy(src, dst, self.send.at[stage], self.recv.at[self.base[stage] + k], dp, self.at["emb"])
        one.start()
        return one

    def start(self, away):
        lo = 1 - self.at["low"] if away else self.at["low"]
        src = self.rows((1 - self.at["par"]) * self.half + lo * self.quarter, self.quarter)
        dst = self.rows(lo * self.quarter, self.quarter)
        one = self.go(self.part.at[src], self.pair.at[dst], 0, 0 if away else 1, self.at["partner"])
        if away:
            self.first_away = one
        else:
            self.first_keep = one

    def stage_x(self):
        at = self.at
        self.first_away.wait_recv()
        self.x = {}
        lo = (1 - at["low"]) * self.quarter
        for k in list(range(1, at["n_hi"])) + [0]:
            piece = at["ahead"][k] * self.size
            mine = self.part[self.rows(at["par"] * self.half + lo + piece, self.size), :]
            theirs = self.pair[self.rows(lo + piece, self.size), :]
            self.x_out[k] = (mine.astype(F32) + theirs.astype(F32)).astype(BF16)
            self.x[k] = self.go(self.x_out.at[k], self.x_in.at[k], 1, k, at["beside"])

    def stage_keep(self):
        at = self.at
        self.first_keep.wait_recv()
        lo = at["low"] * self.quarter
        mine = self.part[self.rows(at["par"] * self.half + lo, self.quarter), :]
        theirs = self.pair[self.rows(lo, self.quarter), :]
        self.keep[...] = mine.astype(F32) + theirs.astype(F32)

    def joined(self, k):
        self.x[k].wait_recv()
        kept = self.keep[self.rows(self.at["ahead"][k] * self.size, self.size), :]
        return kept + self.x_in[k].astype(F32)

    def stage_z(self):
        self.z = []
        for k in range(1, self.at["n_hi"]):
            self.z_out[k - 1] = self.joined(k).astype(BF16)
            self.z.append(
                self.go(self.z_out.at[k - 1], self.z_in.at[k - 1], 2, k - 1, self.at["far"][k])
            )

    def stage_sum(self):
        at = self.at
        total = self.joined(0)
        for k, one in enumerate(self.z):
            one.wait_recv()
            total = total + self.z_in[k].astype(F32)
        self.full[self.place(at["low"], at["high"]), :] = total.astype(BF16)
        self.far, self.near = {}, {}
        for bit in self.bits:
            for sub in range(self.subs):
                self.pass_on(0, sub, bit)
        for sub in range(self.subs):
            self.pass_near(0, sub)

    def pass_on(self, mask, sub, bit):
        at = self.at
        view = self.full.at[self.place(at["low"], flip(at["high"], mask), sub)]
        got = mask | bit
        peer = (2 * flip(at["high"], bit) + at["low"]) * 2 + at["par"]
        self.far[got, sub] = self.go(view, view, 3, self.masks.index(got) * self.subs + sub, peer)

    def pass_near(self, mask, sub):
        at = self.at
        view = self.full.at[self.place(at["low"], flip(at["high"], mask), sub)]
        self.near[mask, sub] = self.go(view, view, 4, mask * self.subs + sub, at["beside"])
        self.go(view, view, 5, 0, at["partner"])

    def take_far(self, mask, sub):
        self.far[mask, sub].wait_recv()
        for bit in self.bits:
            if bit < (mask & -mask):
                self.pass_on(mask, sub, bit)
        self.pass_near(mask, sub)

    def take_near(self, mask, sub):
        self.near[mask, sub].wait_recv()
        view = self.full.at[self.place(1 - self.at["low"], flip(self.at["high"], mask), sub)]
        self.go(view, view, 5, 0, self.at["partner"])

    def spread(self):
        far = [(mask, sub) for mask in self.masks for sub in range(self.subs)]
        near = [(0, sub) for sub in range(self.subs)] + far
        for i, item in enumerate(far):
            self.take_far(*item)
            if i >= self.subs:
                self.take_near(*near[i - self.subs])
        for item in near[len(far) - self.subs :]:
            self.take_near(*item)

    def finish(self):
        partner = self.at["partner"]

        def sizes(ref, stage, k=0):
            return self.copy(ref, ref, self.send.at[stage], self.recv.at[self.base[stage] + k], partner, self.at["emb"])

        whole = self.full.at[self.rows((1 - self.at["par"]) * self.half, self.half)]
        sizes(whole, 5).wait_recv()
        sizes(self.pair, 0).wait_send()
        sizes(self.x_out, 1).wait_send()
        sizes(self.z_out, 2).wait_send()
        sizes(self.z_out, 3).wait_send()
        sizes(self.x_out, 4).wait_send()
        sizes(whole, 5).wait_send()


def flip(index, mask):
    bit = 1
    while bit <= mask:
        if mask & bit:
            index = index + bit * (1 - 2 * ((index // bit) % 2))
        bit *= 2
    return index


def subs_of(size):
    return 2 if size % 256 == 0 else 1


def recv_layout(n_hi, subs):
    counts = [2, n_hi, n_hi - 1, (n_hi - 1) * subs, n_hi * subs, 1]
    starts = [sum(counts[:i]) for i in range(len(counts))]
    return starts, sum(counts)


def tower_kernel(
    n_dp,
    n_emb,
    scale,
    cur_ref,
    prev_ref,
    grads_ref,
    place_ref,
    table_ref,
    labels_ref,
    gain_ref,
    wg_ref,
    wu_ref,
    wo_ref,
    total_ref,
    tower_ref,
    emb_ref,
    ids,
    gall,
    place,
    table,
    labels,
    gain,
    wg,
    wu,
    wo,
    table16,
    wo_row,
    scaled_w,
    contrib,
    lbuf,
    values,
    normed_t,
    act,
    logit_acc,
    logit,
    logit_in,
    slopes,
    lead,
    bn,
    bn_in,
    tpart,
    tpair,
    tx_out,
    tkeep,
    tx_in,
    tz_out,
    tz_in,
    tall,
    gpart,
    gpair,
    gx_out,
    gkeep,
    gx_in,
    gz_out,
    gz_in,
    gall_sum,
    load,
    e_send,
    e_recv,
    t_send,
    t_recv,
    g_send,
    g_recv,
):
    me_dp = lax.axis_index("dp")
    me_emb = lax.axis_index("emb")
    n_chip = n_dp // 2
    n_hi = n_chip // 2
    chip = me_dp // 2
    low = chip % 2
    high = chip // 2
    par = me_dp % 2
    partner = me_dp + 1 - 2 * par
    beside = me_dp + 2 - 4 * low
    tok = gall.shape[1]
    rows = table.shape[0]
    hid = wg.shape[1]
    ht = 256
    tiles = hid // ht

    def copy(src, dst, send, recv, dp, emb):
        return pltpu.make_async_remote_copy(
            src_ref=src,
            dst_ref=dst,
            send_sem=send,
            recv_sem=recv,
            device_id=(dp, emb),
            device_id_type=MESH,
        )

    def other_emb(k):
        return lax.rem(me_emb + k, n_emb)

    def tokens(e):
        return pl.ds(pl.multiple_of(e * tok, tok), tok)

    ahead = [lax.rem(high + k, n_hi) for k in range(n_hi)]
    behind = [lax.rem(high + n_hi - k, n_hi) for k in range(n_hi)]
    far = [(2 * h + low) * 2 + par for h in ahead]
    at = dict(
        n_hi=n_hi, par=par, low=low, high=high, partner=partner, beside=beside,
        ahead=ahead, behind=behind, far=far, emb=me_emb,
    )
    pending = []
    sums = Reduce(
        at, copy, (tpart, tpair, tx_out, tkeep, tx_in, tz_out, tz_in, tall), t_send, t_recv
    )
    tower = Reduce(
        at, copy, (gpart, gpair, gx_out, gkeep, gx_in, gz_out, gz_in, gall_sum), g_send, g_recv
    )

    barrier = pltpu.get_barrier_semaphore()
    for k in range(1, n_emb):
        pl.semaphore_signal(barrier, inc=1, device_id=(me_dp, other_emb(k)), device_id_type=MESH)
    for peer in far[1:] + [beside, partner]:
        pl.semaphore_signal(barrier, inc=1, device_id=(peer, me_emb), device_id_type=MESH)

    loads = []
    for i, (src, dst) in enumerate(
        [
            (cur_ref, ids.at[me_emb, 0]),
            (prev_ref, ids.at[me_emb, 1]),
            (place_ref, place),
            (grads_ref, gall.at[me_emb]),
            (table_ref, table),
            (wo_ref, wo),
            (wg_ref, wg),
            (wu_ref, wu),
            (gain_ref, gain),
            (labels_ref, labels),
        ]
    ):
        one = pltpu.make_async_copy(src, dst, load.at[i])
        one.start()
        loads.append(one)
    loads[0].wait()
    loads[1].wait()
    pl.semaphore_wait(barrier, n_emb - 1 + n_hi - 1 + 2)

    def to_peers(src, dst_of, peers=None):
        sent = []
        for k in peers or range(1, n_emb):
            slot = len(pending)
            one = copy(src, dst_of(k), e_send.at[slot], e_recv.at[slot], me_dp, other_emb(k))
            one.start()
            sent.append(one)
            pending.append(one)
        return sent

    own_ids = ids.at[me_emb]
    id_copies = to_peers(own_ids, lambda k: own_ids)
    loads[3].wait()
    own_grads = gall.at[me_emb]
    grad_copies = to_peers(own_grads, lambda k: own_grads)

    loads[2].wait()
    groups = place.shape[0]
    stored = place[...]
    digits = jnp.concatenate([stored >> 6, stored & 63], axis=0).astype(F32).astype(BF16)

    def place_of(wanted):
        lane = lax.broadcasted_iota(jnp.int32, (LANES, tok), 0)
        hot = jnp.where(lane == (wanted & (LANES - 1)), 1.0, 0.0).astype(BF16)
        found = dot(digits, hot)
        found = found[0:groups, :] * 64.0 + found[groups : 2 * groups, :]
        group = lax.broadcasted_iota(jnp.int32, (groups, tok), 0)
        picked = jnp.where(group == (wanted >> 7), found, 0.0)
        return jnp.sum(picked, axis=0, keepdims=True).astype(jnp.int32)

    base = me_emb * rows
    kt = 256
    prev_pos = []

    loads[4].wait()
    table16[...] = table[...].astype(BF16)

    row_copies = {}
    for s in range(n_emb):
        e = other_emb(s)
        if s > 0:
            id_copies[n_emb - s - 1].wait_recv()
        line = jnp.broadcast_to(place_of(ids[e, 0]) - base, (LANES, tok)).T
        line = jnp.concatenate([line] * (kt // LANES), axis=1)
        acc = jnp.zeros((tok, LANES), F32)
        for i in range(rows // kt):
            index = lax.broadcasted_iota(jnp.int32, (tok, kt), 1) + i * kt
            hot = jnp.where(index == line, 1.0, 0.0).astype(BF16)
            acc = acc + dot(hot, table16[i * kt : (i + 1) * kt, :])
        view = contrib.at[tokens(e)]
        contrib[tokens(e), :] = acc.astype(BF16)
        for k, one in enumerate(to_peers(view, lambda k: lbuf.at[k - 1, tokens(e)])):
            row_copies[k + 1, s] = one
        prev_pos.append((e, place_of(ids[e, 1]) - base))

    for one in grad_copies:
        one.wait_recv()
    half_rows = rows // 2
    pt = 128 if half_rows % 128 == 0 else half_rows

    def grad_half(which):
        for i in range(half_rows // pt):
            at_row = pl.multiple_of(which * half_rows + i * pt, pt)
            index = lax.broadcasted_iota(jnp.int32, (pt, tok), 0) + at_row
            acc = jnp.zeros((pt, LANES), F32)
            for e, pos in prev_pos:
                hot = jnp.where(index == pos, 1.0, 0.0).astype(BF16)
                acc = acc + dot(hot, gall[e])
            tpart[pl.ds(at_row, pt), :] = acc

    grad_half(1 - par)
    sums.start(True)
    sums.start(False)
    grad_half(par)
    for one in loads[5:]:
        one.wait()
    wo_row[...] = wo[...].astype(F32)
    per_tile = ht // LANES

    def head_of(j):
        parts = [wo_row[pl.ds(j * per_tile + b, 1), :] for b in range(per_tile)]
        return jnp.concatenate(parts, axis=1)

    def forward(e):
        span = tokens(e)
        looked = contrib[span, :].astype(F32)
        for k in range(1, n_emb):
            looked = looked + lbuf[k - 1, span, :].astype(F32)
        values[span, :] = looked
        inverse_rms = lax.rsqrt(jnp.mean(looked * looked, axis=1, keepdims=True) + norm_eps)
        norm = (looked * inverse_rms * gain[...]).astype(BF16)
        norm_half = norm * jnp.asarray(0.5, BF16)
        normed_t[:, span] = norm.astype(F32).T
        logit_sum = jnp.zeros((tok, LANES), F32)
        logit_acc[...] = logit_sum
        for j in range(tiles):
            cols = slice(j * ht, (j + 1) * ht)
            half_gate = dot(norm_half, wg[:, cols])
            up = dot(norm, wu[:, cols])
            t = jnp.tanh(half_gate)
            above = 1.0 + t
            risen = up * above
            act[0, span, cols] = (risen * (1.0 + half_gate * (1.0 - t))).astype(BF16)
            act[1, span, cols] = (half_gate * above).astype(BF16)
            weighed = half_gate * risen * head_of(j)
            part = weighed[:, 0:LANES]
            for b in range(1, per_tile):
                part = part + weighed[:, b * LANES : (b + 1) * LANES]
            logit_acc[...] += part
        logit[e] = jnp.sum(logit_acc[...].T, axis=0, keepdims=True)

    logit_copies = []
    for q in range(1, n_emb + 1):
        e = other_emb(n_emb - q)
        for k in range(1, n_emb):
            row_copies[k, (k - q) % n_emb].wait_recv()
        forward(e)
        view = logit.at[e]
        logit_copies += to_peers(view, lambda k: logit_in.at[k - 1, e])
        if q == 1:
            sums.stage_x()
    sums.stage_keep()
    sums.stage_z()

    for one in logit_copies:
        one.wait_recv()
    for e in range(n_emb):
        logits = logit[e]
        for k in range(n_emb - 1):
            logits = logits + logit_in[k, e]
        slope = loss_weight * (jax.nn.sigmoid(logits) - labels[e])
        slopes[e] = slope
        span = slice(e * tok, (e + 1) * tok)
        lead[:, span] = (normed_t[:, span] * slope).astype(BF16)

    def weight_grads(which, lo):
        factor = scale * (0.5 + 0.5 * which.astype(F32))
        for i in range(tiles // 2):
            j = lo * (tiles // 2) + i
            cols = pl.ds(pl.multiple_of(j * ht, ht), ht)
            part = (dot(lead[...], act[which, :, cols]) * (head_of(j) * factor)).astype(BF16)
            for b in range(per_tile):
                to = which * hid + j * ht + b * LANES
                gpart[pl.ds(pl.multiple_of(to, LANES), LANES), :] = part[:, b * LANES : (b + 1) * LANES]

    weight_grads(1 - par, 1 - low)
    tower.start(True)
    weight_grads(par, 1 - low)
    tower.stage_x()
    weight_grads(1 - par, low)
    tower.start(False)
    weight_grads(par, low)
    tower.stage_keep()
    sums.stage_sum()

    for j in range(tiles):
        cols = slice(j * ht, (j + 1) * ht)
        head = head_of(j)
        scaled_w[0, :, cols] = (wg[:, cols].astype(F32) * (0.5 * head)).astype(BF16)
        scaled_w[1, :, cols] = (wu[:, cols].astype(F32) * head).astype(BF16)
    back_copies = []
    for q in range(1, n_emb + 1):
        e = other_emb(n_emb - q)
        span = tokens(e)
        bn[span, :] = dot_nt(act[0, span, :], scaled_w[0]) + dot_nt(act[1, span, :], scaled_w[1])
        if q < n_emb:
            back_copies += to_peers(bn.at[span], lambda k: bn_in.at[k - 1], [n_emb - q])

    tower.stage_z()
    sums.spread()
    tower.stage_sum()

    for one in back_copies:
        one.wait_recv()
    own = tokens(me_emb)
    back = bn[own, :]
    for k in range(n_emb - 1):
        back = back + bn_in[k]
    slope_col = jnp.broadcast_to(slopes[me_emb], (LANES, tok)).T
    scaled = back * slope_col * gain[...]
    x = values[own, :]
    inv = lax.rsqrt(jnp.mean(x * x, axis=1, keepdims=True) + norm_eps)
    emb_ref[...] = inv * scaled - x * (inv * inv * inv) * jnp.mean(
        x * scaled, axis=1, keepdims=True
    )

    tower.spread()
    sums.finish()
    total_ref[...] = tall[...]
    tower.finish()
    tower_ref[...] = gall_sum[...]
    for one in pending:
        one.wait_send()


def write_kernel(
    total_ref, table_ref, accum_ref, tower_ref, emb_ref,
    table_out, accum_out, gate_out, up_out, emb_out,
    new_table, new_accum, gate, up, sem,
):
    hid = gate.shape[1]
    rows = new_table.shape[0]
    sent = []

    def send(src, dst):
        one = pltpu.make_async_copy(src, dst, sem.at[len(sent)])
        one.start()
        sent.append(one)

    send(emb_ref, emb_out)
    n_col = 2
    for which, (buf, out) in enumerate(((gate, gate_out), (up, up_out))):
        for c in range(n_col):
            for b in range(c * hid // LANES // n_col, (c + 1) * hid // LANES // n_col):
                start = which * hid + b * LANES
                buf[:, b * LANES : (b + 1) * LANES] = tower_ref[start : start + LANES, :].astype(F32)
            cols = slice(c * hid // n_col, (c + 1) * hid // n_col)
            send(buf.at[:, cols], out.at[:, cols])
    n_row = 2
    for c in range(n_row):
        span = slice(c * rows // n_row, (c + 1) * rows // n_row)
        total = total_ref[span, :].astype(F32)
        grown = accum_ref[span, :] + total * total
        new_accum[span, :] = grown
        new_table[span, :] = table_ref[span, :] - learn_rate * total * lax.rsqrt(grown)
        send(new_accum.at[span], accum_out.at[span])
        send(new_table.at[span], table_out.at[span])
    for one in sent:
        one.wait()


def on_device(
    cur_ids, prev_ids, prev_grads, row_place, table, accum, labels, gain, w_gate, w_up, w_out
):
    n_emb = lax.axis_size("emb")
    n_dp = lax.axis_size("dp")
    n_chip = n_dp // 2
    n_hi = n_chip // 2
    rows, width = table.shape
    tok = cur_ids.shape[0]
    group = tok * n_emb
    hid = w_gate.shape[1]
    groups = row_place.shape[0] // LANES
    scale = 1.0 / math.sqrt(tok * n_emb * n_dp)
    vmem = pl.BlockSpec(memory_space=pltpu.VMEM)
    hbm = pl.BlockSpec(memory_space=pltpu.HBM)
    n_peer = max(n_emb - 1, 1)
    dma = pltpu.SemaphoreType.DMA
    I32 = jnp.int32
    emb_copies = max((n_emb - 1) * (2 * n_emb + 3), 1)

    def reduce_buffers(total_rows, dtype):
        half = total_rows // 2
        size = half // n_chip
        return [
            pltpu.VMEM((total_rows, width), dtype),
            pltpu.VMEM((half, width), dtype),
            pltpu.VMEM((n_hi, size, width), BF16),
            pltpu.VMEM((half // 2, width), F32),
            pltpu.VMEM((n_hi, size, width), BF16),
            pltpu.VMEM((n_hi - 1, size, width), BF16),
            pltpu.VMEM((n_hi - 1, size, width), BF16),
            pltpu.VMEM((total_rows, width), BF16),
        ]

    total, tower, emb_grad = pl.pallas_call(
        functools.partial(tower_kernel, n_dp, n_emb, scale),
        out_shape=(
            jax.ShapeDtypeStruct((rows, width), BF16),
            jax.ShapeDtypeStruct((2 * hid, width), BF16),
            jax.ShapeDtypeStruct((tok, width), F32),
        ),
        in_specs=[hbm] * 10,
        out_specs=(vmem,) * 3,
        scratch_shapes=[
            pltpu.VMEM((n_emb, 2, 1, tok), I32),
            pltpu.VMEM((n_emb, tok, width), BF16),
            pltpu.VMEM((groups, LANES), I32),
            pltpu.VMEM((rows, width), F32),
            pltpu.VMEM((n_emb, 1, tok), F32),
            pltpu.VMEM((1, width), F32),
            pltpu.VMEM((width, hid), BF16),
            pltpu.VMEM((width, hid), BF16),
            pltpu.VMEM((hid // LANES, LANES), BF16),
            pltpu.VMEM((rows, width), BF16),
            pltpu.VMEM((hid // LANES, LANES), F32),
            pltpu.VMEM((2, width, hid), BF16),
            pltpu.VMEM((group, width), BF16),
            pltpu.VMEM((n_peer, group, width), BF16),
            pltpu.VMEM((group, width), F32),
            pltpu.VMEM((width, group), F32),
            pltpu.VMEM((2, group, hid), BF16),
            pltpu.VMEM((tok, width), F32),
            pltpu.VMEM((n_emb, 1, tok), F32),
            pltpu.VMEM((n_peer, n_emb, 1, tok), F32),
            pltpu.VMEM((n_emb, 1, tok), F32),
            pltpu.VMEM((width, group), BF16),
            pltpu.VMEM((group, width), F32),
            pltpu.VMEM((n_peer, tok, width), F32),
        ]
        + reduce_buffers(rows, F32)
        + reduce_buffers(2 * hid, BF16)
        + [
            dma((10,)),
            dma((emb_copies,)),
            dma((emb_copies,)),
            dma((6,)),
            dma((recv_layout(n_hi, subs_of(rows // 4 // n_hi))[1],)),
            dma((6,)),
            dma((recv_layout(n_hi, subs_of(hid // 2 // n_hi))[1],)),
        ],
        compiler_params=pltpu.CompilerParams(
            collective_id=0, has_side_effects=True, vmem_limit_bytes=40 * 1024 * 1024
        ),
    )(
        *[
            pltpu.with_memory_space_constraint(x, pltpu.HBM)
            for x in (
                cur_ids.reshape(1, -1),
                prev_ids.reshape(1, -1),
                prev_grads,
                row_place.reshape(-1, LANES),
                table,
                labels.reshape(n_emb, 1, -1),
                gain.reshape(1, -1),
                w_gate,
                w_up,
                w_out.reshape(-1, LANES),
            )
        ]
    )
    return pl.pallas_call(
        write_kernel,
        out_shape=(
            jax.ShapeDtypeStruct((rows, width), F32),
            jax.ShapeDtypeStruct((rows, width), F32),
            jax.ShapeDtypeStruct((width, hid), F32),
            jax.ShapeDtypeStruct((width, hid), F32),
            jax.ShapeDtypeStruct((tok, width), F32),
        ),
        in_specs=[vmem] * 5,
        out_specs=(hbm,) * 5,
        scratch_shapes=[
            pltpu.VMEM((rows, width), F32),
            pltpu.VMEM((rows, width), F32),
            pltpu.VMEM((width, hid), F32),
            pltpu.VMEM((width, hid), F32),
            dma((9,)),
        ],
        compiler_params=pltpu.CompilerParams(vmem_limit_bytes=16 * 1024 * 1024),
    )(total, table, accum, tower, emb_grad)


def solution(mesh):
    placed = (
        P(("dp", "emb")),
        P(("dp", "emb")),
        P(("dp", "emb"), None),
        P(),
        P("emb", None),
        P("emb", None),
        P("dp"),
        P(),
        P(None, "emb"),
        P(None, "emb"),
        P("emb"),
    )
    return jax.shard_map(
        on_device,
        mesh=mesh,
        in_specs=placed,
        out_specs=(
            P("emb", None),
            P("emb", None),
            P(None, "emb"),
            P(None, "emb"),
            P(("dp", "emb"), None),
        ),
        check_vma=False,
    )
```

```python
import functools
import math

import jax
import jax.numpy as jnp
from jax import lax
from jax.experimental import pallas as pl
from jax.experimental.pallas import tpu as pltpu
from jax.sharding import PartitionSpec as P

loss_weight = 64.0
learn_rate = 0.1
norm_eps = 1e-06
MESH = pl.DeviceIdType.MESH
F32 = jnp.float32
BF16 = jnp.bfloat16
LANES = 128


def dot(a, b):
    return jnp.dot(a, b, preferred_element_type=F32)


def dot_nt(a, b):
    return lax.dot_general(a, b, (((1,), (1,)), ((), ())), preferred_element_type=F32)


class Reduce:
    def __init__(self, at, copy, bufs, send, recv):
        self.at, self.copy = at, copy
        self.part, self.pair, self.x_out, self.keep, self.x_in, self.z_out, self.z_in, self.full = bufs
        self.send, self.recv = send, recv
        self.half = self.pair.shape[0]
        self.quarter = self.half // 2
        n_hi = at["n_hi"]
        self.size = self.quarter // n_hi
        self.subs = subs_of(self.size)
        self.bits = [1 << b for b in reversed(range(n_hi.bit_length() - 1))]
        self.masks = sorted(range(1, n_hi), key=lambda m: (-(m & -m), m))
        self.base = recv_layout(n_hi, self.subs)[0]

    def rows(self, start, size):
        return pl.ds(pl.multiple_of(start, math.gcd(size, 128)), size)

    def place(self, lo, hi, sub=None):
        start = self.at["par"] * self.half + lo * self.quarter + hi * self.size
        if sub is None:
            return self.rows(start, self.size)
        step = self.size // self.subs
        return self.rows(start + sub * step, step)

    def go(self, src, dst, stage, k, dp):
        one = self.copy(src, dst, self.send.at[stage], self.recv.at[self.base[stage] + k], dp, self.at["emb"])
        one.start()
        return one

    def start(self, away):
        lo = 1 - self.at["low"] if away else self.at["low"]
        src = self.rows((1 - self.at["par"]) * self.half + lo * self.quarter, self.quarter)
        dst = self.rows(lo * self.quarter, self.quarter)
        one = self.go(self.part.at[src], self.pair.at[dst], 0, 0 if away else 1, self.at["partner"])
        if away:
            self.first_away = one
        else:
            self.first_keep = one

    def stage_x(self):
        at = self.at
        self.first_away.wait_recv()
        self.x, self.z = {}, {}
        lo = (1 - at["low"]) * self.quarter
        for k in list(range(1, at["n_hi"])) + [0]:
            piece = at["ahead"][k] * self.size
            mine = self.part[self.rows(at["par"] * self.half + lo + piece, self.size), :]
            theirs = self.pair[self.rows(lo + piece, self.size), :]
            self.x_out[k] = (mine.astype(F32) + theirs.astype(F32)).astype(BF16)
            self.x[k] = self.go(self.x_out.at[k], self.x_in.at[k], 1, k, at["beside"])

    def stage_keep(self):
        at = self.at
        self.first_keep.wait_recv()
        lo = at["low"] * self.quarter
        mine = self.part[self.rows(at["par"] * self.half + lo, self.quarter), :]
        theirs = self.pair[self.rows(lo, self.quarter), :]
        self.keep[...] = mine.astype(F32) + theirs.astype(F32)

    def joined(self, k):
        self.x[k].wait_recv()
        kept = self.keep[self.rows(self.at["ahead"][k] * self.size, self.size), :]
        return kept + self.x_in[k].astype(F32)

    def stage_z(self, k):
        self.z_out[k - 1] = self.joined(k).astype(BF16)
        self.z[k] = self.go(
            self.z_out.at[k - 1], self.z_in.at[k - 1], 2, k - 1, self.at["far"][k]
        )

    def stage_sum(self):
        at = self.at
        total = self.joined(0)
        for k in range(1, at["n_hi"]):
            self.z[k].wait_recv()
            total = total + self.z_in[k - 1].astype(F32)
        self.full[self.place(at["low"], at["high"]), :] = total.astype(BF16)
        self.far, self.near = {}, {}
        for bit in self.bits:
            for sub in range(self.subs):
                self.pass_on(0, sub, bit)
        for sub in range(self.subs):
            self.pass_near(0, sub)

    def pass_on(self, mask, sub, bit):
        at = self.at
        view = self.full.at[self.place(at["low"], flip(at["high"], mask), sub)]
        got = mask | bit
        peer = (2 * flip(at["high"], bit) + at["low"]) * 2 + at["par"]
        self.far[got, sub] = self.go(view, view, 3, self.masks.index(got) * self.subs + sub, peer)

    def pass_near(self, mask, sub):
        at = self.at
        view = self.full.at[self.place(at["low"], flip(at["high"], mask), sub)]
        self.near[mask, sub] = self.go(view, view, 4, mask * self.subs + sub, at["beside"])
        self.go(view, view, 5, 0, at["partner"])

    def take_far(self, mask, sub):
        self.far[mask, sub].wait_recv()
        for bit in self.bits:
            if bit < (mask & -mask):
                self.pass_on(mask, sub, bit)
        self.pass_near(mask, sub)

    def take_near(self, mask, sub):
        self.near[mask, sub].wait_recv()
        view = self.full.at[self.place(1 - self.at["low"], flip(self.at["high"], mask), sub)]
        self.go(view, view, 5, 0, self.at["partner"])

    def spread(self):
        far = [(mask, sub) for mask in self.masks for sub in range(self.subs)]
        near = [(0, sub) for sub in range(self.subs)] + far
        for i, item in enumerate(far):
            self.take_far(*item)
            if i >= self.subs:
                self.take_near(*near[i - self.subs])
        for item in near[len(far) - self.subs :]:
            self.take_near(*item)

    def finish(self):
        partner = self.at["partner"]

        def sizes(ref, stage, k=0):
            return self.copy(ref, ref, self.send.at[stage], self.recv.at[self.base[stage] + k], partner, self.at["emb"])

        whole = self.full.at[self.rows((1 - self.at["par"]) * self.half, self.half)]
        sizes(whole, 5).wait_recv()
        sizes(self.pair, 0).wait_send()
        sizes(self.x_out, 1).wait_send()
        sizes(self.z_out, 2).wait_send()
        sizes(self.z_out, 3).wait_send()
        sizes(self.x_out, 4).wait_send()
        sizes(whole, 5).wait_send()


def flip(index, mask):
    bit = 1
    while bit <= mask:
        if mask & bit:
            index = index + bit * (1 - 2 * ((index // bit) % 2))
        bit *= 2
    return index


def subs_of(size):
    return 4 if size % 256 == 0 else 1


def recv_layout(n_hi, subs):
    counts = [2, n_hi, n_hi - 1, (n_hi - 1) * subs, n_hi * subs, 1]
    starts = [sum(counts[:i]) for i in range(len(counts))]
    return starts, sum(counts)


def tower_kernel(
    n_dp,
    n_emb,
    scale,
    cur_ref,
    prev_ref,
    grads_ref,
    place_ref,
    table_ref,
    labels_ref,
    gain_ref,
    wg_ref,
    wu_ref,
    wo_ref,
    total_ref,
    tower_ref,
    emb_ref,
    ids,
    gall,
    place,
    table,
    labels,
    gain,
    wg,
    wu,
    wo,
    table16,
    wo_row,
    scaled_w,
    contrib,
    lbuf,
    values,
    normed_t,
    act,
    logit_acc,
    logit,
    logit_in,
    slopes,
    lead,
    bn,
    bn_in,
    tpart,
    tpair,
    tx_out,
    tkeep,
    tx_in,
    tz_out,
    tz_in,
    tall,
    gpart,
    gpair,
    gx_out,
    gkeep,
    gx_in,
    gz_out,
    gz_in,
    gall_sum,
    load,
    e_send,
    e_recv,
    t_send,
    t_recv,
    g_send,
    g_recv,
):
    me_dp = lax.axis_index("dp")
    me_emb = lax.axis_index("emb")
    n_chip = n_dp // 2
    n_hi = n_chip // 2
    chip = me_dp // 2
    low = chip % 2
    high = chip // 2
    par = me_dp % 2
    partner = me_dp + 1 - 2 * par
    beside = me_dp + 2 - 4 * low
    tok = gall.shape[1]
    rows = table.shape[0]
    hid = wg.shape[1]
    ht = 256
    tiles = hid // ht

    def copy(src, dst, send, recv, dp, emb):
        return pltpu.make_async_remote_copy(
            src_ref=src,
            dst_ref=dst,
            send_sem=send,
            recv_sem=recv,
            device_id=(dp, emb),
            device_id_type=MESH,
        )

    def other_emb(k):
        return lax.rem(me_emb + k, n_emb)

    def tokens(e):
        return pl.ds(pl.multiple_of(e * tok, tok), tok)

    ahead = [lax.rem(high + k, n_hi) for k in range(n_hi)]
    behind = [lax.rem(high + n_hi - k, n_hi) for k in range(n_hi)]
    far = [(2 * h + low) * 2 + par for h in ahead]
    at = dict(
        n_hi=n_hi, par=par, low=low, high=high, partner=partner, beside=beside,
        ahead=ahead, behind=behind, far=far, emb=me_emb,
    )
    pending = []
    sums = Reduce(
        at, copy, (tpart, tpair, tx_out, tkeep, tx_in, tz_out, tz_in, tall), t_send, t_recv
    )
    tower = Reduce(
        at, copy, (gpart, gpair, gx_out, gkeep, gx_in, gz_out, gz_in, gall_sum), g_send, g_recv
    )

    barrier = pltpu.get_barrier_semaphore()
    for k in range(1, n_emb):
        pl.semaphore_signal(barrier, inc=1, device_id=(me_dp, other_emb(k)), device_id_type=MESH)
    for peer in far[1:] + [beside, partner]:
        pl.semaphore_signal(barrier, inc=1, device_id=(peer, me_emb), device_id_type=MESH)

    loads = []
    for i, (src, dst) in enumerate(
        [
            (cur_ref, ids.at[me_emb, 0]),
            (prev_ref, ids.at[me_emb, 1]),
            (place_ref, place),
            (grads_ref, gall.at[me_emb]),
            (table_ref, table),
            (wo_ref, wo),
            (wg_ref, wg),
            (wu_ref, wu),
            (gain_ref, gain),
            (labels_ref, labels),
        ]
    ):
        one = pltpu.make_async_copy(src, dst, load.at[i])
        one.start()
        loads.append(one)
    loads[0].wait()
    loads[1].wait()
    pl.semaphore_wait(barrier, n_emb - 1 + n_hi - 1 + 2)

    def to_peers(src, dst_of, peers=None):
        sent = []
        for k in peers or range(1, n_emb):
            slot = len(pending)
            one = copy(src, dst_of(k), e_send.at[slot], e_recv.at[slot], me_dp, other_emb(k))
            one.start()
            sent.append(one)
            pending.append(one)
        return sent

    own_ids = ids.at[me_emb]
    id_copies = to_peers(own_ids, lambda k: own_ids)
    loads[2].wait()
    groups = place.shape[0]
    stored = place[...]
    digits = jnp.concatenate([stored >> 6, stored & 63], axis=0).astype(F32).astype(BF16)

    def place_of(wanted):
        lane = lax.broadcasted_iota(jnp.int32, (LANES, tok), 0)
        hot = jnp.where(lane == (wanted & (LANES - 1)), 1.0, 0.0).astype(BF16)
        found = dot(digits, hot)
        found = found[0:groups, :] * 64.0 + found[groups : 2 * groups, :]
        group = lax.broadcasted_iota(jnp.int32, (groups, tok), 0)
        picked = jnp.where(group == (wanted >> 7), found, 0.0)
        return jnp.sum(picked, axis=0, keepdims=True).astype(jnp.int32)

    base = me_emb * rows
    kt = 256
    prev_pos = []

    loads[4].wait()
    table16[...] = table[...].astype(BF16)

    row_copies = {}
    for s in range(n_emb):
        e = other_emb(s)
        if s > 0:
            id_copies[n_emb - s - 1].wait_recv()
        line = jnp.broadcast_to(place_of(ids[e, 0]) - base, (LANES, tok)).T
        line = jnp.concatenate([line] * (kt // LANES), axis=1)
        acc = jnp.zeros((tok, LANES), F32)
        for i in range(rows // kt):
            index = lax.broadcasted_iota(jnp.int32, (tok, kt), 1) + i * kt
            hot = jnp.where(index == line, 1.0, 0.0).astype(BF16)
            acc = acc + dot(hot, table16[i * kt : (i + 1) * kt, :])
        view = contrib.at[tokens(e)]
        contrib[tokens(e), :] = acc.astype(BF16)
        for k, one in enumerate(to_peers(view, lambda k: lbuf.at[k - 1, tokens(e)])):
            row_copies[k + 1, s] = one
        if s == 0:
            loads[3].wait()
            own_grads = gall.at[me_emb]
            grad_copies = to_peers(own_grads, lambda k: own_grads)
        prev_pos.append((e, place_of(ids[e, 1]) - base))

    half_rows = rows // 2
    pt = 128 if half_rows % 128 == 0 else half_rows

    def grad_half(which):
        for i in range(half_rows // pt):
            at_row = pl.multiple_of(which * half_rows + i * pt, pt)
            index = lax.broadcasted_iota(jnp.int32, (pt, tok), 0) + at_row
            acc = jnp.zeros((pt, LANES), F32)
            for e, pos in prev_pos:
                hot = jnp.where(index == pos, 1.0, 0.0).astype(BF16)
                acc = acc + dot(hot, gall[e])
            tpart[pl.ds(at_row, pt), :] = acc

    for one in loads[5:]:
        one.wait()
    wo_row[...] = wo[...].astype(F32)
    per_tile = ht // LANES

    def head_of(j):
        parts = [wo_row[pl.ds(j * per_tile + b, 1), :] for b in range(per_tile)]
        return jnp.concatenate(parts, axis=1)

    def forward(e):
        span = tokens(e)
        looked = contrib[span, :].astype(F32)
        for k in range(1, n_emb):
            looked = looked + lbuf[k - 1, span, :].astype(F32)
        values[span, :] = looked
        inverse_rms = lax.rsqrt(jnp.mean(looked * looked, axis=1, keepdims=True) + norm_eps)
        norm = (looked * inverse_rms * gain[...]).astype(BF16)
        norm_half = norm * jnp.asarray(0.5, BF16)
        normed_t[:, span] = norm.astype(F32).T
        logit_sum = jnp.zeros((tok, LANES), F32)
        logit_acc[...] = logit_sum
        for j in range(tiles):
            cols = slice(j * ht, (j + 1) * ht)
            half_gate = dot(norm_half, wg[:, cols])
            up = dot(norm, wu[:, cols])
            t = jnp.tanh(half_gate)
            above = 1.0 + t
            risen = up * above
            act[0, span, cols] = (risen * (1.0 + half_gate * (1.0 - t))).astype(BF16)
            act[1, span, cols] = (half_gate * above).astype(BF16)
            weighed = half_gate * risen * head_of(j)
            part = weighed[:, 0:LANES]
            for b in range(1, per_tile):
                part = part + weighed[:, b * LANES : (b + 1) * LANES]
            logit_acc[...] += part
        logit[e] = jnp.sum(logit_acc[...].T, axis=0, keepdims=True)

    logit_copies = []
    for q in range(1, n_emb + 1):
        e = other_emb(n_emb - q)
        for k in range(1, n_emb):
            row_copies[k, (k - q) % n_emb].wait_recv()
        forward(e)
        view = logit.at[e]
        logit_copies += to_peers(view, lambda k: logit_in.at[k - 1, e])
        if q == 1:
            for one in grad_copies:
                one.wait_recv()
            grad_half(1 - par)
            sums.start(True)
            sums.start(False)
            grad_half(par)
    sums.stage_x()
    sums.stage_keep()

    for one in logit_copies:
        one.wait_recv()
    for e in range(n_emb):
        logits = logit[e]
        for k in range(n_emb - 1):
            logits = logits + logit_in[k, e]
        slope = loss_weight * (jax.nn.sigmoid(logits) - labels[e])
        slopes[e] = slope
        span = slice(e * tok, (e + 1) * tok)
        lead[:, span] = (normed_t[:, span] * slope).astype(BF16)

    def weight_grads(which, lo):
        factor = scale * (0.5 + 0.5 * which.astype(F32))
        for i in range(tiles // 2):
            j = lo * (tiles // 2) + i
            cols = pl.ds(pl.multiple_of(j * ht, ht), ht)
            part = (dot(lead[...], act[which, :, cols]) * (head_of(j) * factor)).astype(BF16)
            for b in range(per_tile):
                to = which * hid + j * ht + b * LANES
                gpart[pl.ds(pl.multiple_of(to, LANES), LANES), :] = part[:, b * LANES : (b + 1) * LANES]

    weight_grads(1 - par, 1 - low)
    tower.start(True)
    weight_grads(par, 1 - low)
    tower.stage_x()
    for k in range(1, n_hi):
        sums.stage_z(k)
    weight_grads(1 - par, low)
    tower.start(False)
    weight_grads(par, low)
    tower.stage_keep()
    tower.stage_z(1)
    sums.stage_sum()
    for k in range(2, n_hi):
        tower.stage_z(k)

    for j in range(tiles):
        cols = slice(j * ht, (j + 1) * ht)
        head = head_of(j)
        scaled_w[0, :, cols] = (wg[:, cols].astype(F32) * (0.5 * head)).astype(BF16)
        scaled_w[1, :, cols] = (wu[:, cols].astype(F32) * head).astype(BF16)
    back_copies = []
    for q in range(1, n_emb + 1):
        e = other_emb(n_emb - q)
        span = tokens(e)
        bn[span, :] = dot_nt(act[0, span, :], scaled_w[0]) + dot_nt(act[1, span, :], scaled_w[1])
        if q < n_emb:
            back_copies += to_peers(bn.at[span], lambda k: bn_in.at[k - 1], [n_emb - q])

    for mask in sums.masks:
        sums.take_far(mask, 0)
    tower.stage_sum()
    sums.take_near(0, 0)
    for mask in sums.masks:
        sums.take_near(mask, 0)

    for one in back_copies:
        one.wait_recv()
    own = tokens(me_emb)
    back = bn[own, :]
    for k in range(n_emb - 1):
        back = back + bn_in[k]
    slope_col = jnp.broadcast_to(slopes[me_emb], (LANES, tok)).T
    scaled = back * slope_col * gain[...]
    x = values[own, :]
    inv = lax.rsqrt(jnp.mean(x * x, axis=1, keepdims=True) + norm_eps)
    emb_ref[...] = inv * scaled - x * (inv * inv * inv) * jnp.mean(
        x * scaled, axis=1, keepdims=True
    )

    tower.spread()
    sums.finish()
    total_ref[...] = tall[...]
    tower.finish()
    tower_ref[...] = gall_sum[...]
    for one in pending:
        one.wait_send()


def write_kernel(
    total_ref, table_ref, accum_ref, tower_ref, emb_ref,
    table_out, accum_out, gate_out, up_out, emb_out,
    new_table, new_accum, gate, up, sem,
):
    hid = gate.shape[1]
    rows = new_table.shape[0]
    sent = []

    def send(src, dst):
        one = pltpu.make_async_copy(src, dst, sem.at[len(sent)])
        one.start()
        sent.append(one)

    send(emb_ref, emb_out)
    n_col = 2
    for which, (buf, out) in enumerate(((gate, gate_out), (up, up_out))):
        for c in range(n_col):
            for b in range(c * hid // LANES // n_col, (c + 1) * hid // LANES // n_col):
                start = which * hid + b * LANES
                buf[:, b * LANES : (b + 1) * LANES] = tower_ref[start : start + LANES, :].astype(F32)
            cols = slice(c * hid // n_col, (c + 1) * hid // n_col)
            send(buf.at[:, cols], out.at[:, cols])
    n_row = 2
    for c in range(n_row):
        span = slice(c * rows // n_row, (c + 1) * rows // n_row)
        total = total_ref[span, :].astype(F32)
        grown = accum_ref[span, :] + total * total
        new_accum[span, :] = grown
        new_table[span, :] = table_ref[span, :] - learn_rate * total * lax.rsqrt(grown)
        send(new_accum.at[span], accum_out.at[span])
        send(new_table.at[span], table_out.at[span])
    for one in sent:
        one.wait()


def on_device(
    cur_ids, prev_ids, prev_grads, row_place, table, accum, labels, gain, w_gate, w_up, w_out
):
    n_emb = lax.axis_size("emb")
    n_dp = lax.axis_size("dp")
    n_chip = n_dp // 2
    n_hi = n_chip // 2
    rows, width = table.shape
    tok = cur_ids.shape[0]
    group = tok * n_emb
    hid = w_gate.shape[1]
    groups = row_place.shape[0] // LANES
    scale = 1.0 / math.sqrt(tok * n_emb * n_dp)
    vmem = pl.BlockSpec(memory_space=pltpu.VMEM)
    hbm = pl.BlockSpec(memory_space=pltpu.HBM)
    n_peer = max(n_emb - 1, 1)
    dma = pltpu.SemaphoreType.DMA
    I32 = jnp.int32
    emb_copies = max((n_emb - 1) * (2 * n_emb + 3), 1)

    def reduce_buffers(total_rows, dtype):
        half = total_rows // 2
        size = half // n_chip
        return [
            pltpu.VMEM((total_rows, width), dtype),
            pltpu.VMEM((half, width), dtype),
            pltpu.VMEM((n_hi, size, width), BF16),
            pltpu.VMEM((half // 2, width), F32),
            pltpu.VMEM((n_hi, size, width), BF16),
            pltpu.VMEM((n_hi - 1, size, width), BF16),
            pltpu.VMEM((n_hi - 1, size, width), BF16),
            pltpu.VMEM((total_rows, width), BF16),
        ]

    total, tower, emb_grad = pl.pallas_call(
        functools.partial(tower_kernel, n_dp, n_emb, scale),
        out_shape=(
            jax.ShapeDtypeStruct((rows, width), BF16),
            jax.ShapeDtypeStruct((2 * hid, width), BF16),
            jax.ShapeDtypeStruct((tok, width), F32),
        ),
        in_specs=[hbm] * 10,
        out_specs=(vmem,) * 3,
        scratch_shapes=[
            pltpu.VMEM((n_emb, 2, 1, tok), I32),
            pltpu.VMEM((n_emb, tok, width), BF16),
            pltpu.VMEM((groups, LANES), I32),
            pltpu.VMEM((rows, width), F32),
            pltpu.VMEM((n_emb, 1, tok), F32),
            pltpu.VMEM((1, width), F32),
            pltpu.VMEM((width, hid), BF16),
            pltpu.VMEM((width, hid), BF16),
            pltpu.VMEM((hid // LANES, LANES), BF16),
            pltpu.VMEM((rows, width), BF16),
            pltpu.VMEM((hid // LANES, LANES), F32),
            pltpu.VMEM((2, width, hid), BF16),
            pltpu.VMEM((group, width), BF16),
            pltpu.VMEM((n_peer, group, width), BF16),
            pltpu.VMEM((group, width), F32),
            pltpu.VMEM((width, group), F32),
            pltpu.VMEM((2, group, hid), BF16),
            pltpu.VMEM((tok, width), F32),
            pltpu.VMEM((n_emb, 1, tok), F32),
            pltpu.VMEM((n_peer, n_emb, 1, tok), F32),
            pltpu.VMEM((n_emb, 1, tok), F32),
            pltpu.VMEM((width, group), BF16),
            pltpu.VMEM((group, width), F32),
            pltpu.VMEM((n_peer, tok, width), F32),
        ]
        + reduce_buffers(rows, F32)
        + reduce_buffers(2 * hid, BF16)
        + [
            dma((10,)),
            dma((emb_copies,)),
            dma((emb_copies,)),
            dma((6,)),
            dma((recv_layout(n_hi, subs_of(rows // 4 // n_hi))[1],)),
            dma((6,)),
            dma((recv_layout(n_hi, subs_of(hid // 2 // n_hi))[1],)),
        ],
        compiler_params=pltpu.CompilerParams(
            collective_id=0, has_side_effects=True, vmem_limit_bytes=40 * 1024 * 1024
        ),
    )(
        *[
            pltpu.with_memory_space_constraint(x, pltpu.HBM)
            for x in (
                cur_ids.reshape(1, -1),
                prev_ids.reshape(1, -1),
                prev_grads,
                row_place.reshape(-1, LANES),
                table,
                labels.reshape(n_emb, 1, -1),
                gain.reshape(1, -1),
                w_gate,
                w_up,
                w_out.reshape(-1, LANES),
            )
        ]
    )
    return pl.pallas_call(
        write_kernel,
        out_shape=(
            jax.ShapeDtypeStruct((rows, width), F32),
            jax.ShapeDtypeStruct((rows, width), F32),
            jax.ShapeDtypeStruct((width, hid), F32),
            jax.ShapeDtypeStruct((width, hid), F32),
            jax.ShapeDtypeStruct((tok, width), F32),
        ),
        in_specs=[vmem] * 5,
        out_specs=(hbm,) * 5,
        scratch_shapes=[
            pltpu.VMEM((rows, width), F32),
            pltpu.VMEM((rows, width), F32),
            pltpu.VMEM((width, hid), F32),
            pltpu.VMEM((width, hid), F32),
            dma((9,)),
        ],
        compiler_params=pltpu.CompilerParams(vmem_limit_bytes=16 * 1024 * 1024),
    )(total, table, accum, tower, emb_grad)


def solution(mesh):
    placed = (
        P(("dp", "emb")),
        P(("dp", "emb")),
        P(("dp", "emb"), None),
        P(),
        P("emb", None),
        P("emb", None),
        P("dp"),
        P(),
        P(None, "emb"),
        P(None, "emb"),
        P("emb"),
    )
    return jax.shard_map(
        on_device,
        mesh=mesh,
        in_specs=placed,
        out_specs=(
            P("emb", None),
            P("emb", None),
            P(None, "emb"),
            P(None, "emb"),
            P(("dp", "emb"), None),
        ),
        check_vma=False,
    )
```

```python
import functools
import math

import jax
import jax.numpy as jnp
from jax import lax
from jax.experimental import pallas as pl
from jax.experimental.pallas import tpu as pltpu
from jax.sharding import PartitionSpec as P

loss_weight = 64.0
learn_rate = 0.1
norm_eps = 1e-06
MESH = pl.DeviceIdType.MESH
F32 = jnp.float32
BF16 = jnp.bfloat16
LANES = 128


def dot(a, b):
    return jnp.dot(a, b, preferred_element_type=F32)


def dot_nt(a, b):
    return lax.dot_general(a, b, (((1,), (1,)), ((), ())), preferred_element_type=F32)


class Reduce:
    def __init__(self, at, copy, bufs, send, recv):
        self.at, self.copy = at, copy
        self.part, self.pair, self.x_out, self.keep, self.x_in, self.z_out, self.z_in, self.full = bufs
        self.send, self.recv = send, recv
        n_hi = at["n_hi"]
        self.half = self.part.shape[0] // 2
        self.size = self.half // n_hi
        self.subs = subs_of(self.size)
        self.step = self.size // self.subs
        self.bits = [1 << b for b in reversed(range(n_hi.bit_length() - 1))]
        self.masks = sorted(range(1, n_hi), key=lambda m: (-(m & -m), m))
        self.order = list(range(1, n_hi)) + [0]
        self.base = recv_layout(n_hi, self.subs)[0]

    def rows(self, start, size):
        return pl.ds(pl.multiple_of(start, math.gcd(size, 128)), size)

    def place(self, lo, hi, sub=None):
        start = lo * self.half + hi * self.size
        if sub is None:
            return self.rows(start, self.size)
        return self.rows(start + sub * self.step, self.step)

    def go(self, src, dst, stage, k, dp):
        self.copy(src, dst, self.send.at[stage], self.recv.at[self.base[stage] + k], dp, self.at["emb"]).start()

    def waiter(self, ref, stage, k=0):
        return self.copy(
            ref, ref, self.send.at[stage], self.recv.at[self.base[stage] + k], self.at["partner"], self.at["emb"]
        )

    def got(self, ref, stage, k):
        self.waiter(ref, stage, k).wait_recv()

    def start(self, k):
        at = self.at
        piece = self.place(1 - at["low"], at["ahead"][k])
        self.go(self.part.at[piece], self.pair.at[piece], 0, k, at["partner"])

    def start_keep(self):
        at = self.at
        kept = self.rows(at["low"] * self.half, self.half)
        self.go(self.part.at[kept], self.pair.at[kept], 0, at["n_hi"], at["partner"])

    def stage_x(self, k):
        at = self.at
        self.got(self.pair.at[0 : self.size], 0, k)
        piece = self.place(1 - at["low"], at["ahead"][k])
        both = self.part[piece, :].astype(F32) + self.pair[piece, :].astype(F32)
        self.x_out[k] = both.astype(BF16)
        self.go(self.x_out.at[k], self.x_in.at[k], 1, k, at["beside"])

    def stage_keep(self):
        at = self.at
        self.got(self.pair.at[0 : self.half], 0, at["n_hi"])
        kept = self.rows(at["low"] * self.half, self.half)
        self.keep[...] = self.part[kept, :].astype(F32) + self.pair[kept, :].astype(F32)

    def joined(self, k):
        self.got(self.x_in.at[k], 1, k)
        kept = self.keep[self.rows(self.at["ahead"][k] * self.size, self.size), :]
        return kept + self.x_in[k].astype(F32)

    def stage_z(self, k):
        self.z_out[k - 1] = self.joined(k).astype(BF16)
        self.go(self.z_out.at[k - 1], self.z_in.at[k - 1], 2, k - 1, self.at["far"][k])

    def stage_sum(self):
        at = self.at
        total = self.joined(0)
        for k in range(1, at["n_hi"]):
            self.got(self.z_in.at[k - 1], 2, k - 1)
            total = total + self.z_in[k - 1].astype(F32)
        self.full[self.place(at["low"], at["high"]), :] = total.astype(BF16)
        for bit in self.bits:
            for sub in range(self.subs):
                self.pass_on(0, sub, bit)
        for sub in range(self.subs):
            self.pass_near(0, sub)

    def pass_on(self, mask, sub, bit):
        at = self.at
        view = self.full.at[self.place(at["low"], flip(at["high"], mask), sub)]
        peer = (2 * flip(at["high"], bit) + at["low"]) * 2 + at["par"]
        self.go(view, view, 3, self.masks.index(mask | bit) * self.subs + sub, peer)

    def pass_near(self, mask, sub):
        at = self.at
        view = self.full.at[self.place(at["low"], flip(at["high"], mask), sub)]
        self.go(view, view, 4, mask * self.subs + sub, at["beside"])
        self.go(view, view, 5, 0, at["partner"])

    def take_far(self, mask, sub):
        self.got(self.full.at[0 : self.step], 3, self.masks.index(mask) * self.subs + sub)
        for bit in self.bits:
            if bit < (mask & -mask):
                self.pass_on(mask, sub, bit)
        self.pass_near(mask, sub)

    def take_near(self, mask, sub):
        self.got(self.full.at[0 : self.step], 4, mask * self.subs + sub)
        view = self.full.at[self.place(1 - self.at["low"], flip(self.at["high"], mask), sub)]
        self.go(view, view, 5, 0, self.at["partner"])

    def spread(self):
        far = [(mask, sub) for mask in self.masks for sub in range(self.subs)]
        near = [(0, sub) for sub in range(self.subs)] + far
        for i, item in enumerate(far):
            self.take_far(*item)
            if i >= self.subs:
                self.take_near(*near[i - self.subs])
        for item in near[len(far) - self.subs :]:
            self.take_near(*item)

    def finish_owner(self):
        self.waiter(self.x_out, 1).wait_send()
        self.waiter(self.z_out, 2).wait_send()
        self.waiter(self.z_out, 3).wait_send()
        self.waiter(self.x_out, 4).wait_send()
        self.waiter(self.full, 5).wait_send()

    def finish_other(self):
        self.waiter(self.pair, 0).wait_send()
        self.got(self.full, 5, 0)


def flip(index, mask):
    bit = 1
    while bit <= mask:
        if mask & bit:
            index = index + bit * (1 - 2 * ((index // bit) % 2))
        bit *= 2
    return index


def subs_of(size):
    return 4 if size % 256 == 0 else 1


def recv_layout(n_hi, subs):
    counts = [n_hi + 1, n_hi, n_hi - 1, (n_hi - 1) * subs, n_hi * subs, 1]
    starts = [sum(counts[:i]) for i in range(len(counts))]
    return starts, sum(counts)


def tower_kernel(
    n_dp,
    n_emb,
    scale,
    cur_ref,
    prev_ref,
    grads_ref,
    place_ref,
    table_ref,
    labels_ref,
    gain_ref,
    wg_ref,
    wu_ref,
    wo_ref,
    total_ref,
    tower_ref,
    emb_ref,
    ids,
    gall,
    place,
    table,
    labels,
    gain,
    wg,
    wu,
    wo,
    table16,
    wo_row,
    scaled_w,
    contrib,
    lbuf,
    values,
    normed_t,
    act,
    logit_acc,
    logit,
    logit_in,
    slopes,
    lead,
    bn,
    bn_in,
    tpart,
    tpair,
    tx_out,
    tkeep,
    tx_in,
    tz_out,
    tz_in,
    tall,
    gpart,
    gpair,
    gx_out,
    gkeep,
    gx_in,
    gz_out,
    gz_in,
    gall_sum,
    load,
    e_send,
    e_recv,
    t_send,
    t_recv,
    g_send,
    g_recv,
):
    me_dp = lax.axis_index("dp")
    me_emb = lax.axis_index("emb")
    n_chip = n_dp // 2
    n_hi = n_chip // 2
    chip = me_dp // 2
    low = chip % 2
    high = chip // 2
    par = me_dp % 2
    partner = me_dp + 1 - 2 * par
    beside = me_dp + 2 - 4 * low
    tok = gall.shape[1]
    rows = table.shape[0]
    hid = wg.shape[1]
    ht = 256
    tiles = hid // ht

    def copy(src, dst, send, recv, dp, emb):
        return pltpu.make_async_remote_copy(
            src_ref=src,
            dst_ref=dst,
            send_sem=send,
            recv_sem=recv,
            device_id=(dp, emb),
            device_id_type=MESH,
        )

    def other_emb(k):
        return lax.rem(me_emb + k, n_emb)

    def tokens(e):
        return pl.ds(pl.multiple_of(e * tok, tok), tok)

    ahead = [lax.rem(high + k, n_hi) for k in range(n_hi)]
    behind = [lax.rem(high + n_hi - k, n_hi) for k in range(n_hi)]
    far = [(2 * h + low) * 2 + par for h in ahead]
    at = dict(
        n_hi=n_hi, par=par, low=low, high=high, partner=partner, beside=beside,
        ahead=ahead, behind=behind, far=far, emb=me_emb,
    )
    pending = []
    sums = Reduce(
        at, copy, (tpart, tpair, tx_out, tkeep, tx_in, tz_out, tz_in, tall), t_send, t_recv
    )
    tower = Reduce(
        at, copy, (gpart, gpair, gx_out, gkeep, gx_in, gz_out, gz_in, gall_sum), g_send, g_recv
    )

    barrier = pltpu.get_barrier_semaphore()
    for k in range(1, n_emb):
        pl.semaphore_signal(barrier, inc=1, device_id=(me_dp, other_emb(k)), device_id_type=MESH)
    for peer in far[1:] + [beside, partner]:
        pl.semaphore_signal(barrier, inc=1, device_id=(peer, me_emb), device_id_type=MESH)

    loads = []
    for i, (src, dst) in enumerate(
        [
            (cur_ref, ids.at[me_emb, 0]),
            (prev_ref, ids.at[me_emb, 1]),
            (place_ref, place),
            (grads_ref, gall.at[me_emb]),
            (table_ref, table),
            (wo_ref, wo),
            (wg_ref, wg),
            (wu_ref, wu),
            (gain_ref, gain),
            (labels_ref, labels),
        ]
    ):
        one = pltpu.make_async_copy(src, dst, load.at[i])
        one.start()
        loads.append(one)
    loads[0].wait()
    loads[1].wait()
    pl.semaphore_wait(barrier, n_emb - 1 + n_hi - 1 + 2)

    def to_peers(src, dst_of, peers=None):
        sent = []
        for k in peers or range(1, n_emb):
            slot = len(pending)
            one = copy(src, dst_of(k), e_send.at[slot], e_recv.at[slot], me_dp, other_emb(k))
            one.start()
            sent.append(one)
            pending.append(one)
        return sent

    own_ids = ids.at[me_emb]
    id_copies = to_peers(own_ids, lambda k: own_ids)
    loads[2].wait()
    groups = place.shape[0]
    stored = place[...]
    digits = jnp.concatenate([stored >> 6, stored & 63], axis=0).astype(F32).astype(BF16)

    def place_of(wanted):
        lane = lax.broadcasted_iota(jnp.int32, (LANES, tok), 0)
        hot = jnp.where(lane == (wanted & (LANES - 1)), 1.0, 0.0).astype(BF16)
        found = dot(digits, hot)
        found = found[0:groups, :] * 64.0 + found[groups : 2 * groups, :]
        group = lax.broadcasted_iota(jnp.int32, (groups, tok), 0)
        picked = jnp.where(group == (wanted >> 7), found, 0.0)
        return jnp.sum(picked, axis=0, keepdims=True).astype(jnp.int32)

    base = me_emb * rows
    kt = 256
    prev_pos = []

    loads[4].wait()
    table16[...] = table[...].astype(BF16)

    row_copies = {}
    for s in range(n_emb):
        e = other_emb(s)
        if s > 0:
            id_copies[n_emb - s - 1].wait_recv()
        line = jnp.broadcast_to(place_of(ids[e, 0]) - base, (LANES, tok)).T
        line = jnp.concatenate([line] * (kt // LANES), axis=1)
        acc = jnp.zeros((tok, LANES), F32)
        for i in range(rows // kt):
            index = lax.broadcasted_iota(jnp.int32, (tok, kt), 1) + i * kt
            hot = jnp.where(index == line, 1.0, 0.0).astype(BF16)
            acc = acc + dot(hot, table16[i * kt : (i + 1) * kt, :])
        view = contrib.at[tokens(e)]
        contrib[tokens(e), :] = acc.astype(BF16)
        for k, one in enumerate(to_peers(view, lambda k: lbuf.at[k - 1, tokens(e)])):
            row_copies[k + 1, s] = one
        if s == 0:
            loads[3].wait()
            own_grads = gall.at[me_emb]
            grad_copies = to_peers(own_grads, lambda k: own_grads)
        prev_pos.append((e, place_of(ids[e, 1]) - base))

    pt = 128 if rows % 128 == 0 else rows

    def table_sums():
        for i in range(rows // pt):
            index = lax.broadcasted_iota(jnp.int32, (pt, tok), 0) + i * pt
            acc = jnp.zeros((pt, LANES), F32)
            for e, pos in prev_pos:
                hot = jnp.where(index == pos, 1.0, 0.0).astype(BF16)
                acc = acc + dot(hot, gall[e])
            tpart[i * pt : (i + 1) * pt, :] = acc

    for one in loads[5:]:
        one.wait()
    wo_row[...] = wo[...].astype(F32)
    per_tile = ht // LANES

    def head_of(j):
        parts = [wo_row[pl.ds(j * per_tile + b, 1), :] for b in range(per_tile)]
        return jnp.concatenate(parts, axis=1)

    def forward(e):
        span = tokens(e)
        looked = contrib[span, :].astype(F32)
        for k in range(1, n_emb):
            looked = looked + lbuf[k - 1, span, :].astype(F32)
        values[span, :] = looked
        inverse_rms = lax.rsqrt(jnp.mean(looked * looked, axis=1, keepdims=True) + norm_eps)
        norm = (looked * inverse_rms * gain[...]).astype(BF16)
        norm_half = norm * jnp.asarray(0.5, BF16)
        normed_t[:, span] = norm.astype(F32).T
        logit_sum = jnp.zeros((tok, LANES), F32)
        logit_acc[...] = logit_sum
        for j in range(tiles):
            cols = slice(j * ht, (j + 1) * ht)
            half_gate = dot(norm_half, wg[:, cols])
            up = dot(norm, wu[:, cols])
            t = jnp.tanh(half_gate)
            above = 1.0 + t
            risen = up * above
            act[0, span, cols] = (risen * (1.0 + half_gate * (1.0 - t))).astype(BF16)
            act[1, span, cols] = (half_gate * above).astype(BF16)
            weighed = half_gate * risen * head_of(j)
            part = weighed[:, 0:LANES]
            for b in range(1, per_tile):
                part = part + weighed[:, b * LANES : (b + 1) * LANES]
            logit_acc[...] += part
        logit[e] = jnp.sum(logit_acc[...].T, axis=0, keepdims=True)

    logit_copies = []
    for q in range(1, n_emb + 1):
        e = other_emb(n_emb - q)
        for k in range(1, n_emb):
            row_copies[k, (k - q) % n_emb].wait_recv()
        forward(e)
        view = logit.at[e]
        logit_copies += to_peers(view, lambda k: logit_in.at[k - 1, e])
        if q == 1:
            for one in grad_copies:
                one.wait_recv()
            table_sums()

            @pl.when(par == 1)
            def _():
                for k in sums.order:
                    sums.start(k)
                sums.start_keep()

    @pl.when(par == 0)
    def _():
        for k in sums.order:
            sums.stage_x(k)
        sums.stage_keep()

    for one in logit_copies:
        one.wait_recv()
    for e in range(n_emb):
        logits = logit[e]
        for k in range(n_emb - 1):
            logits = logits + logit_in[k, e]
        slope = loss_weight * (jax.nn.sigmoid(logits) - labels[e])
        slopes[e] = slope
        span = slice(e * tok, (e + 1) * tok)
        lead[:, span] = (normed_t[:, span] * slope).astype(BF16)

    def weight_block(which, col, width, to):
        factor = scale * (0.5 + 0.5 * which)
        heads = [wo_row[pl.ds(col // LANES + b, 1), :] for b in range(width // LANES)]
        head = jnp.concatenate(heads, axis=1) * factor
        cols = pl.ds(pl.multiple_of(col, width), width)
        part = (dot(lead[...], act[which, :, cols]) * head).astype(BF16)
        for b in range(width // LANES):
            gpart[pl.ds(pl.multiple_of(to + b * LANES, LANES), LANES), :] = part[
                :, b * LANES : (b + 1) * LANES
            ]

    side = hid // 2

    def weight_side(lo):
        width = min(ht, side)
        for which in range(2):
            for i in range(side // width):
                weight_block(which, lo * side + i * width, width, lo * hid + which * side + i * width)

    by_piece = tower.size % LANES == 0 and side % tower.size == 0

    def weight_piece(k):
        if not by_piece:
            if k == tower.order[0]:
                weight_side(1 - low)
            return
        width = min(ht, tower.size)
        first = at["ahead"][k] * tower.size
        which = first // side
        for i in range(tower.size // width):
            col = (1 - low) * side + first % side + i * width
            weight_block(which, col, width, (1 - low) * hid + first + i * width)

    back_slot = len(pending)

    def back_copy(k):
        span = tokens(other_emb(k))
        slot = back_slot + k - 1
        return copy(bn.at[span], bn_in.at[k - 1], e_send.at[slot], e_recv.at[slot], me_dp, other_emb(k))

    def backward():
        for j in range(tiles):
            cols = slice(j * ht, (j + 1) * ht)
            head = head_of(j)
            scaled_w[0, :, cols] = (wg[:, cols].astype(F32) * (0.5 * head)).astype(BF16)
            scaled_w[1, :, cols] = (wu[:, cols].astype(F32) * head).astype(BF16)
        for k in range(n_emb - 1, -1, -1):
            span = tokens(other_emb(k))
            bn[span, :] = dot_nt(act[0, span, :], scaled_w[0]) + dot_nt(act[1, span, :], scaled_w[1])
            if k > 0:
                back_copy(k).start()

    def embed():
        for k in range(1, n_emb):
            back_copy(k).wait()
        own = tokens(me_emb)
        back = bn[own, :]
        for k in range(n_emb - 1):
            back = back + bn_in[k]
        slope_col = jnp.broadcast_to(slopes[me_emb], (LANES, tok)).T
        scaled = back * slope_col * gain[...]
        x = values[own, :]
        inv = lax.rsqrt(jnp.mean(x * x, axis=1, keepdims=True) + norm_eps)
        emb_ref[...] = inv * scaled - x * (inv * inv * inv) * jnp.mean(
            x * scaled, axis=1, keepdims=True
        )

    @pl.when(par == 1)
    def _():
        for i, k in enumerate(tower.order):
            weight_piece(k)
            if i > 0:
                tower.stage_x(tower.order[i - 1])
        tower.stage_x(tower.order[-1])
        weight_side(low)
        tower.stage_keep()
        for k in range(1, n_hi):
            tower.stage_z(k)
        backward()
        tower.stage_sum()
        embed()
        tower.spread()
        tower_ref[...] = gall_sum[...]
        sums.finish_other()
        total_ref[...] = tall[...]
        tower.finish_owner()

    @pl.when(par == 0)
    def _():
        for k in tower.order:
            weight_piece(k)
            tower.start(k)
        weight_side(low)
        tower.start_keep()
        for k in range(1, n_hi):
            sums.stage_z(k)
        backward()
        sums.stage_sum()
        embed()
        sums.spread()
        total_ref[...] = tall[...]
        sums.finish_owner()
        tower.finish_other()
        tower_ref[...] = gall_sum[...]

    for one in pending:
        one.wait_send()


def write_kernel(
    total_ref, table_ref, accum_ref, tower_ref, emb_ref,
    table_out, accum_out, gate_out, up_out, emb_out,
    new_table, new_accum, gate, up, sem,
):
    hid = gate.shape[1]
    rows = new_table.shape[0]
    sent = []

    def send(src, dst):
        one = pltpu.make_async_copy(src, dst, sem.at[len(sent)])
        one.start()
        sent.append(one)

    send(emb_ref, emb_out)
    n_col = 2
    for which, (buf, out) in enumerate(((gate, gate_out), (up, up_out))):
        for c in range(n_col):
            for b in range(c * hid // LANES // n_col, (c + 1) * hid // LANES // n_col):
                half_blocks = hid // LANES // 2
                start = (b // half_blocks) * hid + which * (hid // 2) + b % half_blocks * LANES
                buf[:, b * LANES : (b + 1) * LANES] = tower_ref[start : start + LANES, :].astype(F32)
            cols = slice(c * hid // n_col, (c + 1) * hid // n_col)
            send(buf.at[:, cols], out.at[:, cols])
    n_row = 2
    for c in range(n_row):
        span = slice(c * rows // n_row, (c + 1) * rows // n_row)
        total = total_ref[span, :].astype(F32)
        grown = accum_ref[span, :] + total * total
        new_accum[span, :] = grown
        new_table[span, :] = table_ref[span, :] - learn_rate * total * lax.rsqrt(grown)
        send(new_accum.at[span], accum_out.at[span])
        send(new_table.at[span], table_out.at[span])
    for one in sent:
        one.wait()


def on_device(
    cur_ids, prev_ids, prev_grads, row_place, table, accum, labels, gain, w_gate, w_up, w_out
):
    n_emb = lax.axis_size("emb")
    n_dp = lax.axis_size("dp")
    n_chip = n_dp // 2
    n_hi = n_chip // 2
    rows, width = table.shape
    tok = cur_ids.shape[0]
    group = tok * n_emb
    hid = w_gate.shape[1]
    groups = row_place.shape[0] // LANES
    scale = 1.0 / math.sqrt(tok * n_emb * n_dp)
    vmem = pl.BlockSpec(memory_space=pltpu.VMEM)
    hbm = pl.BlockSpec(memory_space=pltpu.HBM)
    n_peer = max(n_emb - 1, 1)
    dma = pltpu.SemaphoreType.DMA
    I32 = jnp.int32
    emb_copies = max((n_emb - 1) * (2 * n_emb + 3), 1)

    def reduce_buffers(total_rows, dtype):
        half = total_rows // 2
        size = half // n_hi
        return [
            pltpu.VMEM((total_rows, width), dtype),
            pltpu.VMEM((total_rows, width), dtype),
            pltpu.VMEM((n_hi, size, width), BF16),
            pltpu.VMEM((half, width), F32),
            pltpu.VMEM((n_hi, size, width), BF16),
            pltpu.VMEM((n_hi - 1, size, width), BF16),
            pltpu.VMEM((n_hi - 1, size, width), BF16),
            pltpu.VMEM((total_rows, width), BF16),
        ]

    total, tower, emb_grad = pl.pallas_call(
        functools.partial(tower_kernel, n_dp, n_emb, scale),
        out_shape=(
            jax.ShapeDtypeStruct((rows, width), BF16),
            jax.ShapeDtypeStruct((2 * hid, width), BF16),
            jax.ShapeDtypeStruct((tok, width), F32),
        ),
        in_specs=[hbm] * 10,
        out_specs=(vmem,) * 3,
        scratch_shapes=[
            pltpu.VMEM((n_emb, 2, 1, tok), I32),
            pltpu.VMEM((n_emb, tok, width), BF16),
            pltpu.VMEM((groups, LANES), I32),
            pltpu.VMEM((rows, width), F32),
            pltpu.VMEM((n_emb, 1, tok), F32),
            pltpu.VMEM((1, width), F32),
            pltpu.VMEM((width, hid), BF16),
            pltpu.VMEM((width, hid), BF16),
            pltpu.VMEM((hid // LANES, LANES), BF16),
            pltpu.VMEM((rows, width), BF16),
            pltpu.VMEM((hid // LANES, LANES), F32),
            pltpu.VMEM((2, width, hid), BF16),
            pltpu.VMEM((group, width), BF16),
            pltpu.VMEM((n_peer, group, width), BF16),
            pltpu.VMEM((group, width), F32),
            pltpu.VMEM((width, group), F32),
            pltpu.VMEM((2, group, hid), BF16),
            pltpu.VMEM((tok, width), F32),
            pltpu.VMEM((n_emb, 1, tok), F32),
            pltpu.VMEM((n_peer, n_emb, 1, tok), F32),
            pltpu.VMEM((n_emb, 1, tok), F32),
            pltpu.VMEM((width, group), BF16),
            pltpu.VMEM((group, width), F32),
            pltpu.VMEM((n_peer, tok, width), F32),
        ]
        + reduce_buffers(rows, F32)
        + reduce_buffers(2 * hid, BF16)
        + [
            dma((10,)),
            dma((emb_copies,)),
            dma((emb_copies,)),
            dma((6,)),
            dma((recv_layout(n_hi, subs_of(rows // 2 // n_hi))[1],)),
            dma((6,)),
            dma((recv_layout(n_hi, subs_of(hid // n_hi))[1],)),
        ],
        compiler_params=pltpu.CompilerParams(
            collective_id=0, has_side_effects=True, vmem_limit_bytes=40 * 1024 * 1024
        ),
    )(
        *[
            pltpu.with_memory_space_constraint(x, pltpu.HBM)
            for x in (
                cur_ids.reshape(1, -1),
                prev_ids.reshape(1, -1),
                prev_grads,
                row_place.reshape(-1, LANES),
                table,
                labels.reshape(n_emb, 1, -1),
                gain.reshape(1, -1),
                w_gate,
                w_up,
                w_out.reshape(-1, LANES),
            )
        ]
    )
    return pl.pallas_call(
        write_kernel,
        out_shape=(
            jax.ShapeDtypeStruct((rows, width), F32),
            jax.ShapeDtypeStruct((rows, width), F32),
            jax.ShapeDtypeStruct((width, hid), F32),
            jax.ShapeDtypeStruct((width, hid), F32),
            jax.ShapeDtypeStruct((tok, width), F32),
        ),
        in_specs=[vmem] * 5,
        out_specs=(hbm,) * 5,
        scratch_shapes=[
            pltpu.VMEM((rows, width), F32),
            pltpu.VMEM((rows, width), F32),
            pltpu.VMEM((width, hid), F32),
            pltpu.VMEM((width, hid), F32),
            dma((9,)),
        ],
        compiler_params=pltpu.CompilerParams(vmem_limit_bytes=16 * 1024 * 1024),
    )(total, table, accum, tower, emb_grad)


def solution(mesh):
    placed = (
        P(("dp", "emb")),
        P(("dp", "emb")),
        P(("dp", "emb"), None),
        P(),
        P("emb", None),
        P("emb", None),
        P("dp"),
        P(),
        P(None, "emb"),
        P(None, "emb"),
        P("emb"),
    )
    return jax.shard_map(
        on_device,
        mesh=mesh,
        in_specs=placed,
        out_specs=(
            P("emb", None),
            P("emb", None),
            P(None, "emb"),
            P(None, "emb"),
            P(("dp", "emb"), None),
        ),
        check_vma=False,
    )
```

```python
import functools
import math

import jax
import jax.numpy as jnp
from jax import lax
from jax.experimental import pallas as pl
from jax.experimental.pallas import tpu as pltpu
from jax.sharding import PartitionSpec as P

loss_weight = 64.0
learn_rate = 0.1
norm_eps = 1e-06
MESH = pl.DeviceIdType.MESH
F32 = jnp.float32
BF16 = jnp.bfloat16
LANES = 128


def dot(a, b):
    return jnp.dot(a, b, preferred_element_type=F32)


def dot_nt(a, b):
    return lax.dot_general(a, b, (((1,), (1,)), ((), ())), preferred_element_type=F32)


class Reduce:
    def __init__(self, at, copy, bufs, send, recv):
        self.at, self.copy = at, copy
        self.part, self.pair, self.x_out, self.keep, self.x_in, self.z_out, self.z_in, self.full = bufs
        self.send, self.recv = send, recv
        n_hi = at["n_hi"]
        self.half = self.part.shape[0] // 2
        self.size = self.half // n_hi
        self.subs = subs_of(self.size)
        self.step = self.size // self.subs
        self.bits = [1 << b for b in reversed(range(n_hi.bit_length() - 1))]
        self.masks = sorted(range(1, n_hi), key=lambda m: (-(m & -m), m))
        self.order = list(range(1, n_hi)) + [0]
        self.base = recv_layout(n_hi, self.subs)[0]

    def rows(self, start, size):
        return pl.ds(pl.multiple_of(start, math.gcd(size, 128)), size)

    def place(self, lo, hi, sub=None):
        start = lo * self.half + hi * self.size
        if sub is None:
            return self.rows(start, self.size)
        return self.rows(start + sub * self.step, self.step)

    def go(self, src, dst, stage, k, dp):
        self.copy(src, dst, self.send.at[stage], self.recv.at[self.base[stage] + k], dp, self.at["emb"]).start()

    def waiter(self, ref, stage, k=0):
        return self.copy(
            ref, ref, self.send.at[stage], self.recv.at[self.base[stage] + k], self.at["partner"], self.at["emb"]
        )

    def got(self, ref, stage, k):
        self.waiter(ref, stage, k).wait_recv()

    def start(self, k):
        at = self.at
        piece = self.place(1 - at["low"], at["ahead"][k])
        self.go(self.part.at[piece], self.pair.at[piece], 0, k, at["partner"])

    def start_keep(self):
        at = self.at
        kept = self.rows(at["low"] * self.half, self.half)
        self.go(self.part.at[kept], self.pair.at[kept], 0, at["n_hi"], at["partner"])

    def stage_x(self, k):
        at = self.at
        self.got(self.pair.at[0 : self.size], 0, k)
        piece = self.place(1 - at["low"], at["ahead"][k])
        both = self.part[piece, :].astype(F32) + self.pair[piece, :].astype(F32)
        self.x_out[k] = both.astype(BF16)
        self.go(self.x_out.at[k], self.x_in.at[k], 1, k, at["beside"])

    def stage_keep(self):
        at = self.at
        self.got(self.pair.at[0 : self.half], 0, at["n_hi"])
        kept = self.rows(at["low"] * self.half, self.half)
        self.keep[...] = self.part[kept, :].astype(F32) + self.pair[kept, :].astype(F32)

    def joined(self, k):
        self.got(self.x_in.at[k], 1, k)
        kept = self.keep[self.rows(self.at["ahead"][k] * self.size, self.size), :]
        return kept + self.x_in[k].astype(F32)

    def stage_z(self, k):
        self.z_out[k - 1] = self.joined(k).astype(BF16)
        self.go(self.z_out.at[k - 1], self.z_in.at[k - 1], 2, k - 1, self.at["far"][k])

    def stage_sum(self):
        at = self.at
        total = self.joined(0)
        for k in range(1, at["n_hi"]):
            self.got(self.z_in.at[k - 1], 2, k - 1)
            total = total + self.z_in[k - 1].astype(F32)
        self.full[self.place(at["low"], at["high"]), :] = total.astype(BF16)
        for bit in self.bits:
            for sub in range(self.subs):
                self.pass_on(0, sub, bit)
        for sub in range(self.subs):
            self.pass_near(0, sub)

    def pass_on(self, mask, sub, bit):
        at = self.at
        view = self.full.at[self.place(at["low"], flip(at["high"], mask), sub)]
        peer = (2 * flip(at["high"], bit) + at["low"]) * 2 + at["par"]
        self.go(view, view, 3, self.masks.index(mask | bit) * self.subs + sub, peer)

    def pass_near(self, mask, sub):
        at = self.at
        view = self.full.at[self.place(at["low"], flip(at["high"], mask), sub)]
        self.go(view, view, 4, mask * self.subs + sub, at["beside"])
        self.go(view, view, 5, 0, at["partner"])

    def take_far(self, mask, sub):
        self.got(self.full.at[0 : self.step], 3, self.masks.index(mask) * self.subs + sub)
        for bit in self.bits:
            if bit < (mask & -mask):
                self.pass_on(mask, sub, bit)
        self.pass_near(mask, sub)

    def take_near(self, mask, sub):
        self.got(self.full.at[0 : self.step], 4, mask * self.subs + sub)
        view = self.full.at[self.place(1 - self.at["low"], flip(self.at["high"], mask), sub)]
        self.go(view, view, 5, 0, self.at["partner"])

    def spread(self):
        far = [(mask, sub) for mask in self.masks for sub in range(self.subs)]
        near = [(0, sub) for sub in range(self.subs)] + far
        for i, item in enumerate(far):
            self.take_far(*item)
            if i >= self.subs:
                self.take_near(*near[i - self.subs])
        for item in near[len(far) - self.subs :]:
            self.take_near(*item)

    def finish_owner(self):
        self.waiter(self.x_out, 1).wait_send()
        self.waiter(self.z_out, 2).wait_send()
        self.waiter(self.z_out, 3).wait_send()
        self.waiter(self.x_out, 4).wait_send()
        self.waiter(self.full, 5).wait_send()

    def finish_other(self):
        self.waiter(self.pair, 0).wait_send()
        self.got(self.full, 5, 0)


def flip(index, mask):
    bit = 1
    while bit <= mask:
        if mask & bit:
            index = index + bit * (1 - 2 * ((index // bit) % 2))
        bit *= 2
    return index


def subs_of(size):
    return 8 if size % 256 == 0 else 1


def recv_layout(n_hi, subs):
    counts = [n_hi + 1, n_hi, n_hi - 1, (n_hi - 1) * subs, n_hi * subs, 1]
    starts = [sum(counts[:i]) for i in range(len(counts))]
    return starts, sum(counts)


def tower_kernel(
    n_dp,
    n_emb,
    scale,
    cur_ref,
    prev_ref,
    grads_ref,
    place_ref,
    table_ref,
    labels_ref,
    gain_ref,
    wg_ref,
    wu_ref,
    wo_ref,
    total_ref,
    tower_ref,
    emb_ref,
    ids,
    gall,
    place,
    table,
    labels,
    gain,
    wg,
    wu,
    wo,
    table16,
    wo_row,
    scaled_w,
    contrib,
    lbuf,
    values,
    normed_t,
    act,
    logit_acc,
    logit,
    logit_in,
    slopes,
    lead,
    bn,
    bn_in,
    tpart,
    tpair,
    tx_out,
    tkeep,
    tx_in,
    tz_out,
    tz_in,
    tall,
    gpart,
    gpair,
    gx_out,
    gkeep,
    gx_in,
    gz_out,
    gz_in,
    gall_sum,
    load,
    e_send,
    e_recv,
    t_send,
    t_recv,
    g_send,
    g_recv,
):
    me_dp = lax.axis_index("dp")
    me_emb = lax.axis_index("emb")
    n_chip = n_dp // 2
    n_hi = n_chip // 2
    chip = me_dp // 2
    low = chip % 2
    high = chip // 2
    par = me_dp % 2
    partner = me_dp + 1 - 2 * par
    beside = me_dp + 2 - 4 * low
    tok = gall.shape[1]
    rows = table.shape[0]
    hid = wg.shape[1]
    ht = 256
    tiles = hid // ht

    def copy(src, dst, send, recv, dp, emb):
        return pltpu.make_async_remote_copy(
            src_ref=src,
            dst_ref=dst,
            send_sem=send,
            recv_sem=recv,
            device_id=(dp, emb),
            device_id_type=MESH,
        )

    def other_emb(k):
        return lax.rem(me_emb + k, n_emb)

    def tokens(e):
        return pl.ds(pl.multiple_of(e * tok, tok), tok)

    ahead = [lax.rem(high + k, n_hi) for k in range(n_hi)]
    behind = [lax.rem(high + n_hi - k, n_hi) for k in range(n_hi)]
    far = [(2 * h + low) * 2 + par for h in ahead]
    at = dict(
        n_hi=n_hi, par=par, low=low, high=high, partner=partner, beside=beside,
        ahead=ahead, behind=behind, far=far, emb=me_emb,
    )
    pending = []
    sums = Reduce(
        at, copy, (tpart, tpair, tx_out, tkeep, tx_in, tz_out, tz_in, tall), t_send, t_recv
    )
    tower = Reduce(
        at, copy, (gpart, gpair, gx_out, gkeep, gx_in, gz_out, gz_in, gall_sum), g_send, g_recv
    )

    barrier = pltpu.get_barrier_semaphore()
    for k in range(1, n_emb):
        pl.semaphore_signal(barrier, inc=1, device_id=(me_dp, other_emb(k)), device_id_type=MESH)
    for peer in far[1:] + [beside, partner]:
        pl.semaphore_signal(barrier, inc=1, device_id=(peer, me_emb), device_id_type=MESH)

    loads = []
    for i, (src, dst) in enumerate(
        [
            (cur_ref, ids.at[me_emb, 0]),
            (prev_ref, ids.at[me_emb, 1]),
            (place_ref, place),
            (grads_ref, gall.at[me_emb]),
            (table_ref, table),
            (wo_ref, wo),
            (wg_ref, wg),
            (wu_ref, wu),
            (gain_ref, gain),
            (labels_ref, labels),
        ]
    ):
        one = pltpu.make_async_copy(src, dst, load.at[i])
        one.start()
        loads.append(one)
    loads[0].wait()
    loads[1].wait()
    pl.semaphore_wait(barrier, n_emb - 1 + n_hi - 1 + 2)

    def to_peers(src, dst_of, peers=None):
        sent = []
        for k in peers or range(1, n_emb):
            slot = len(pending)
            one = copy(src, dst_of(k), e_send.at[slot], e_recv.at[slot], me_dp, other_emb(k))
            one.start()
            sent.append(one)
            pending.append(one)
        return sent

    own_ids = ids.at[me_emb]
    id_copies = to_peers(own_ids, lambda k: own_ids)
    loads[3].wait()
    own_grads = gall.at[me_emb]
    grad_copies = to_peers(own_grads, lambda k: own_grads)
    loads[2].wait()
    groups = place.shape[0]
    stored = place[...]
    digits = jnp.concatenate([stored >> 6, stored & 63], axis=0).astype(F32).astype(BF16)

    def place_of(wanted):
        lane = lax.broadcasted_iota(jnp.int32, (LANES, tok), 0)
        hot = jnp.where(lane == (wanted & (LANES - 1)), 1.0, 0.0).astype(BF16)
        found = dot(digits, hot)
        found = found[0:groups, :] * 64.0 + found[groups : 2 * groups, :]
        group = lax.broadcasted_iota(jnp.int32, (groups, tok), 0)
        picked = jnp.where(group == (wanted >> 7), found, 0.0)
        return jnp.sum(picked, axis=0, keepdims=True).astype(jnp.int32)

    base = me_emb * rows
    kt = 256
    prev_pos = []

    loads[4].wait()
    table16[...] = table[...].astype(BF16)

    row_copies = {}
    for s in range(n_emb):
        e = other_emb(s)
        if s > 0:
            id_copies[n_emb - s - 1].wait_recv()
        line = jnp.broadcast_to(place_of(ids[e, 0]) - base, (LANES, tok)).T
        line = jnp.concatenate([line] * (kt // LANES), axis=1)
        acc = jnp.zeros((tok, LANES), F32)
        for i in range(rows // kt):
            index = lax.broadcasted_iota(jnp.int32, (tok, kt), 1) + i * kt
            hot = jnp.where(index == line, 1.0, 0.0).astype(BF16)
            acc = acc + dot(hot, table16[i * kt : (i + 1) * kt, :])
        view = contrib.at[tokens(e)]
        contrib[tokens(e), :] = acc.astype(BF16)
        for k, one in enumerate(to_peers(view, lambda k: lbuf.at[k - 1, tokens(e)])):
            row_copies[k + 1, s] = one
        prev_pos.append((e, place_of(ids[e, 1]) - base))

    half_rows = rows // 2
    pt = 128 if half_rows % 128 == 0 else half_rows

    def table_sums(lo):
        for i in range(half_rows // pt):
            at_row = pl.multiple_of(lo * half_rows + i * pt, pt)
            index = lax.broadcasted_iota(jnp.int32, (pt, tok), 0) + at_row
            acc = jnp.zeros((pt, LANES), F32)
            for e, pos in prev_pos:
                hot = jnp.where(index == pos, 1.0, 0.0).astype(BF16)
                acc = acc + dot(hot, gall[e])
            tpart[pl.ds(at_row, pt), :] = acc.astype(BF16)

    for one in grad_copies:
        one.wait_recv()
    table_sums(1 - low)

    @pl.when(par == 1)
    def _():
        for k in sums.order:
            sums.start(k)

    table_sums(low)

    @pl.when(par == 1)
    def _():
        sums.start_keep()

    for one in loads[5:]:
        one.wait()
    wo_row[...] = wo[...].astype(F32)
    per_tile = ht // LANES

    def head_of(j):
        parts = [wo_row[pl.ds(j * per_tile + b, 1), :] for b in range(per_tile)]
        return jnp.concatenate(parts, axis=1)

    def forward(e):
        span = tokens(e)
        looked = contrib[span, :].astype(F32)
        for k in range(1, n_emb):
            looked = looked + lbuf[k - 1, span, :].astype(F32)
        values[span, :] = looked
        inverse_rms = lax.rsqrt(jnp.mean(looked * looked, axis=1, keepdims=True) + norm_eps)
        norm = (looked * inverse_rms * gain[...]).astype(BF16)
        norm_half = norm * jnp.asarray(0.5, BF16)
        normed_t[:, span] = norm.astype(F32).T
        logit_sum = jnp.zeros((tok, LANES), F32)
        logit_acc[...] = logit_sum
        for j in range(tiles):
            cols = slice(j * ht, (j + 1) * ht)
            half_gate = dot(norm_half, wg[:, cols])
            up = dot(norm, wu[:, cols])
            t = jnp.tanh(half_gate)
            above = 1.0 + t
            risen = up * above
            act[0, span, cols] = (risen * (1.0 + half_gate * (1.0 - t))).astype(BF16)
            act[1, span, cols] = (half_gate * above).astype(BF16)
            weighed = half_gate * risen * head_of(j)
            part = weighed[:, 0:LANES]
            for b in range(1, per_tile):
                part = part + weighed[:, b * LANES : (b + 1) * LANES]
            logit_acc[...] += part
        logit[e] = jnp.sum(logit_acc[...].T, axis=0, keepdims=True)

    logit_copies = []
    for q in range(1, n_emb + 1):
        e = other_emb(n_emb - q)
        for k in range(1, n_emb):
            row_copies[k, (k - q) % n_emb].wait_recv()
        forward(e)
        view = logit.at[e]
        logit_copies += to_peers(view, lambda k: logit_in.at[k - 1, e])
        if q == 1:

            @pl.when(par == 0)
            def _():
                for k in sums.order:
                    sums.stage_x(k)

    @pl.when(par == 0)
    def _():
        sums.stage_keep()

    for one in logit_copies:
        one.wait_recv()
    for e in range(n_emb):
        logits = logit[e]
        for k in range(n_emb - 1):
            logits = logits + logit_in[k, e]
        slope = loss_weight * (jax.nn.sigmoid(logits) - labels[e])
        slopes[e] = slope
        span = slice(e * tok, (e + 1) * tok)
        lead[:, span] = (normed_t[:, span] * slope).astype(BF16)

    def weight_block(which, col, width, to):
        factor = scale * (0.5 + 0.5 * which)
        heads = [wo_row[pl.ds(col // LANES + b, 1), :] for b in range(width // LANES)]
        head = jnp.concatenate(heads, axis=1) * factor
        cols = pl.ds(pl.multiple_of(col, width), width)
        part = (dot(lead[...], act[which, :, cols]) * head).astype(BF16)
        for b in range(width // LANES):
            gpart[pl.ds(pl.multiple_of(to + b * LANES, LANES), LANES), :] = part[
                :, b * LANES : (b + 1) * LANES
            ]

    side = hid // 2

    def weight_side(lo):
        width = min(ht, side)
        for which in range(2):
            for i in range(side // width):
                weight_block(which, lo * side + i * width, width, lo * hid + which * side + i * width)

    by_piece = tower.size % LANES == 0 and side % tower.size == 0

    def weight_piece(k):
        if not by_piece:
            if k == tower.order[0]:
                weight_side(1 - low)
            return
        width = min(ht, tower.size)
        first = at["ahead"][k] * tower.size
        which = first // side
        for i in range(tower.size // width):
            col = (1 - low) * side + first % side + i * width
            weight_block(which, col, width, (1 - low) * hid + first + i * width)

    back_slot = len(pending)

    def back_copy(k):
        span = tokens(other_emb(k))
        slot = back_slot + k - 1
        return copy(bn.at[span], bn_in.at[k - 1], e_send.at[slot], e_recv.at[slot], me_dp, other_emb(k))

    def backward():
        for j in range(tiles):
            cols = slice(j * ht, (j + 1) * ht)
            head = head_of(j)
            scaled_w[0, :, cols] = (wg[:, cols].astype(F32) * (0.5 * head)).astype(BF16)
            scaled_w[1, :, cols] = (wu[:, cols].astype(F32) * head).astype(BF16)
        for k in range(n_emb - 1, -1, -1):
            span = tokens(other_emb(k))
            bn[span, :] = dot_nt(act[0, span, :], scaled_w[0]) + dot_nt(act[1, span, :], scaled_w[1])
            if k > 0:
                back_copy(k).start()

    def embed():
        for k in range(1, n_emb):
            back_copy(k).wait()
        own = tokens(me_emb)
        back = bn[own, :]
        for k in range(n_emb - 1):
            back = back + bn_in[k]
        slope_col = jnp.broadcast_to(slopes[me_emb], (LANES, tok)).T
        scaled = back * slope_col * gain[...]
        x = values[own, :]
        inv = lax.rsqrt(jnp.mean(x * x, axis=1, keepdims=True) + norm_eps)
        emb_ref[...] = inv * scaled - x * (inv * inv * inv) * jnp.mean(
            x * scaled, axis=1, keepdims=True
        )

    @pl.when(par == 1)
    def _():
        for i, k in enumerate(tower.order):
            weight_piece(k)
            if i > 0:
                tower.stage_x(tower.order[i - 1])
        tower.stage_x(tower.order[-1])
        weight_side(low)
        tower.stage_keep()
        for k in range(1, n_hi):
            tower.stage_z(k)
        backward()
        tower.stage_sum()
        embed()
        tower.spread()
        tower_ref[...] = gall_sum[...]
        sums.finish_other()
        total_ref[...] = tall[...]
        tower.finish_owner()

    @pl.when(par == 0)
    def _():
        for k in tower.order:
            weight_piece(k)
            tower.start(k)
        for k in range(1, n_hi):
            sums.stage_z(k)
        weight_side(low)
        tower.start_keep()
        backward()
        sums.stage_sum()
        embed()
        sums.spread()
        total_ref[...] = tall[...]
        sums.finish_owner()
        tower.finish_other()
        tower_ref[...] = gall_sum[...]

    for one in pending:
        one.wait_send()


def write_kernel(
    total_ref, table_ref, accum_ref, tower_ref, emb_ref,
    table_out, accum_out, gate_out, up_out, emb_out,
    new_table, new_accum, gate, up, sem,
):
    hid = gate.shape[1]
    rows = new_table.shape[0]
    sent = []

    def send(src, dst):
        one = pltpu.make_async_copy(src, dst, sem.at[len(sent)])
        one.start()
        sent.append(one)

    send(emb_ref, emb_out)
    n_col = 2
    for which, (buf, out) in enumerate(((gate, gate_out), (up, up_out))):
        for c in range(n_col):
            for b in range(c * hid // LANES // n_col, (c + 1) * hid // LANES // n_col):
                half_blocks = hid // LANES // 2
                start = (b // half_blocks) * hid + which * (hid // 2) + b % half_blocks * LANES
                buf[:, b * LANES : (b + 1) * LANES] = tower_ref[start : start + LANES, :].astype(F32)
            cols = slice(c * hid // n_col, (c + 1) * hid // n_col)
            send(buf.at[:, cols], out.at[:, cols])
    n_row = 2
    for c in range(n_row):
        span = slice(c * rows // n_row, (c + 1) * rows // n_row)
        total = total_ref[span, :].astype(F32)
        grown = accum_ref[span, :] + total * total
        new_accum[span, :] = grown
        new_table[span, :] = table_ref[span, :] - learn_rate * total * lax.rsqrt(grown)
        send(new_accum.at[span], accum_out.at[span])
        send(new_table.at[span], table_out.at[span])
    for one in sent:
        one.wait()


def on_device(
    cur_ids, prev_ids, prev_grads, row_place, table, accum, labels, gain, w_gate, w_up, w_out
):
    n_emb = lax.axis_size("emb")
    n_dp = lax.axis_size("dp")
    n_chip = n_dp // 2
    n_hi = n_chip // 2
    rows, width = table.shape
    tok = cur_ids.shape[0]
    group = tok * n_emb
    hid = w_gate.shape[1]
    groups = row_place.shape[0] // LANES
    scale = 1.0 / math.sqrt(tok * n_emb * n_dp)
    vmem = pl.BlockSpec(memory_space=pltpu.VMEM)
    hbm = pl.BlockSpec(memory_space=pltpu.HBM)
    n_peer = max(n_emb - 1, 1)
    dma = pltpu.SemaphoreType.DMA
    I32 = jnp.int32
    emb_copies = max((n_emb - 1) * (2 * n_emb + 3), 1)

    def reduce_buffers(total_rows, dtype):
        half = total_rows // 2
        size = half // n_hi
        return [
            pltpu.VMEM((total_rows, width), dtype),
            pltpu.VMEM((total_rows, width), dtype),
            pltpu.VMEM((n_hi, size, width), BF16),
            pltpu.VMEM((half, width), F32),
            pltpu.VMEM((n_hi, size, width), BF16),
            pltpu.VMEM((n_hi - 1, size, width), BF16),
            pltpu.VMEM((n_hi - 1, size, width), BF16),
            pltpu.VMEM((total_rows, width), BF16),
        ]

    total, tower, emb_grad = pl.pallas_call(
        functools.partial(tower_kernel, n_dp, n_emb, scale),
        out_shape=(
            jax.ShapeDtypeStruct((rows, width), BF16),
            jax.ShapeDtypeStruct((2 * hid, width), BF16),
            jax.ShapeDtypeStruct((tok, width), F32),
        ),
        in_specs=[hbm] * 10,
        out_specs=(vmem,) * 3,
        scratch_shapes=[
            pltpu.VMEM((n_emb, 2, 1, tok), I32),
            pltpu.VMEM((n_emb, tok, width), BF16),
            pltpu.VMEM((groups, LANES), I32),
            pltpu.VMEM((rows, width), F32),
            pltpu.VMEM((n_emb, 1, tok), F32),
            pltpu.VMEM((1, width), F32),
            pltpu.VMEM((width, hid), BF16),
            pltpu.VMEM((width, hid), BF16),
            pltpu.VMEM((hid // LANES, LANES), BF16),
            pltpu.VMEM((rows, width), BF16),
            pltpu.VMEM((hid // LANES, LANES), F32),
            pltpu.VMEM((2, width, hid), BF16),
            pltpu.VMEM((group, width), BF16),
            pltpu.VMEM((n_peer, group, width), BF16),
            pltpu.VMEM((group, width), F32),
            pltpu.VMEM((width, group), F32),
            pltpu.VMEM((2, group, hid), BF16),
            pltpu.VMEM((tok, width), F32),
            pltpu.VMEM((n_emb, 1, tok), F32),
            pltpu.VMEM((n_peer, n_emb, 1, tok), F32),
            pltpu.VMEM((n_emb, 1, tok), F32),
            pltpu.VMEM((width, group), BF16),
            pltpu.VMEM((group, width), F32),
            pltpu.VMEM((n_peer, tok, width), F32),
        ]
        + reduce_buffers(rows, BF16)
        + reduce_buffers(2 * hid, BF16)
        + [
            dma((10,)),
            dma((emb_copies,)),
            dma((emb_copies,)),
            dma((6,)),
            dma((recv_layout(n_hi, subs_of(rows // 2 // n_hi))[1],)),
            dma((6,)),
            dma((recv_layout(n_hi, subs_of(hid // n_hi))[1],)),
        ],
        compiler_params=pltpu.CompilerParams(
            collective_id=0, has_side_effects=True, vmem_limit_bytes=40 * 1024 * 1024
        ),
    )(
        *[
            pltpu.with_memory_space_constraint(x, pltpu.HBM)
            for x in (
                cur_ids.reshape(1, -1),
                prev_ids.reshape(1, -1),
                prev_grads,
                row_place.reshape(-1, LANES),
                table,
                labels.reshape(n_emb, 1, -1),
                gain.reshape(1, -1),
                w_gate,
                w_up,
                w_out.reshape(-1, LANES),
            )
        ]
    )
    return pl.pallas_call(
        write_kernel,
        out_shape=(
            jax.ShapeDtypeStruct((rows, width), F32),
            jax.ShapeDtypeStruct((rows, width), F32),
            jax.ShapeDtypeStruct((width, hid), F32),
            jax.ShapeDtypeStruct((width, hid), F32),
            jax.ShapeDtypeStruct((tok, width), F32),
        ),
        in_specs=[vmem] * 5,
        out_specs=(hbm,) * 5,
        scratch_shapes=[
            pltpu.VMEM((rows, width), F32),
            pltpu.VMEM((rows, width), F32),
            pltpu.VMEM((width, hid), F32),
            pltpu.VMEM((width, hid), F32),
            dma((9,)),
        ],
        compiler_params=pltpu.CompilerParams(vmem_limit_bytes=16 * 1024 * 1024),
    )(total, table, accum, tower, emb_grad)


def solution(mesh):
    placed = (
        P(("dp", "emb")),
        P(("dp", "emb")),
        P(("dp", "emb"), None),
        P(),
        P("emb", None),
        P("emb", None),
        P("dp"),
        P(),
        P(None, "emb"),
        P(None, "emb"),
        P("emb"),
    )
    return jax.shard_map(
        on_device,
        mesh=mesh,
        in_specs=placed,
        out_specs=(
            P("emb", None),
            P("emb", None),
            P(None, "emb"),
            P(None, "emb"),
            P(("dp", "emb"), None),
        ),
        check_vma=False,
    )
```
